8 devices in a mesh: dp: 1 (over z), tp: 2 (over y), cp: 4 (over x, core).
Axes of the slice: x: 2, y: 2, z: 1, core: 2. Of those that a mesh axis runs over, the one named last changes fastest.
Arguments:
- x: bfloat16 [8192, 1536], P(('dp', 'cp', 'tp'))
- pos: int32 [8192], P(('dp', 'cp', 'tp'))
- g1: bfloat16 [1536], replicated
- g2: bfloat16 [1536], replicated
- wq: bfloat16 [1536, 1536], P(None, 'tp')
- wk: bfloat16 [1536, 256], P(None, 'tp')
- wv: bfloat16 [1536, 256], P(None, 'tp')
- wo: bfloat16 [1536, 1536], P('tp')
- w1: bfloat16 [1536, 8960], P(None, 'tp')
- w3: bfloat16 [1536, 8960], P(None, 'tp')
- w2: bfloat16 [8960, 1536], P('tp')
Outputs:
- output: bfloat16 [8192, 1536], P(('dp', 'cp', 'tp'))
All inputs are finite; a program needn't handle non-finite values.
Results may differ from the reference program's by a relative error of at most 0.00963285.
Values are sent between devices in bfloat16 or wider.
A program may use at most 1 GiB of HBM per device.

```python
import math
import jax
import jax.numpy as jnp
from jax import lax

T = 8192
D = 1536
HQ = 12
HKV = 2
DH = 128
F = 8960
NDEV = 8
QB = 64
PIECE = T // (2 * NDEV)
GRP = HQ // HKV
EPS = 1e-5
THETA = 500000.0


def setup_inputs(seed: int = 0, part: int = 0) -> dict:
    kpart = jax.random.fold_in(jax.random.key(seed), part)
    kx, kgap, kstart = jax.random.split(kpart, 3)
    kw = jax.random.split(jax.random.key(seed + 1), 9)
    x = jax.random.normal(kx, (T, D), jnp.float32).astype(jnp.bfloat16)
    gaps = jax.random.randint(kgap, (T,), 1, 4)
    start = jax.random.randint(kstart, (), 0, T)
    seqpos = start + jnp.cumsum(gaps) - gaps[0]
    rows = jnp.arange(T)
    dev = rows // (2 * PIECE)
    off = rows % (2 * PIECE)
    piece = jnp.where(off < PIECE, dev, 2 * NDEV - 1 - dev)
    pos = seqpos[piece * PIECE + off % PIECE].astype(jnp.int32)
    qk = math.sqrt(math.sqrt(math.log(T / 16.0)))

    def nrm(k, shape, scl):
        return (jax.random.normal(k, shape, jnp.float32) * scl).astype(jnp.bfloat16)

    g1 = (1.0 + 0.3 * jax.random.normal(kw[0], (D,), jnp.float32)).astype(jnp.bfloat16)
    g2 = (1.0 + 0.3 * jax.random.normal(kw[1], (D,), jnp.float32)).astype(jnp.bfloat16)
    wq = nrm(kw[2], (D, HQ * DH), qk / math.sqrt(D))
    wk = nrm(kw[3], (D, HKV * DH), qk / math.sqrt(D))
    wv = nrm(kw[4], (D, HKV * DH), 1.0 / math.sqrt(D))
    wo = nrm(kw[5], (HQ * DH, D), 2.0 / math.sqrt(HQ * DH))
    w1 = nrm(kw[6], (D, F), 1.0 / math.sqrt(D))
    w3 = nrm(kw[7], (D, F), 1.0 / math.sqrt(D))
    w2 = nrm(kw[8], (F, D), 1.0 / math.sqrt(F))
    return dict(x=x, pos=pos, g1=g1, g2=g2, wq=wq, wk=wk, wv=wv, wo=wo, w1=w1, w3=w3, w2=w2)


def rms_norm(v, g):
    vf = v.astype(jnp.float32)
    inv = lax.rsqrt(jnp.mean(vf * vf, axis=-1, keepdims=True) + EPS)
    return (vf * inv * g.astype(jnp.float32)).astype(jnp.bfloat16)


def rope(y, p):
    half = DH // 2
    freq = 1.0 / (THETA ** (jnp.arange(0, DH, 2, dtype=jnp.float32) / DH))
    ang = p.astype(jnp.float32)[..., None] * freq
    c = jnp.cos(ang)[..., None, :]
    s = jnp.sin(ang)[..., None, :]
    y1 = y[..., :half]
    y2 = y[..., half:]
    return jnp.concatenate([y1 * c - y2 * s, y2 * c + y1 * s], axis=-1)


def attention(q, k, v, p):
    qr = q.reshape(T // QB, QB, HKV, GRP, DH)
    pr = p.reshape(T // QB, QB)
    kf = k.astype(jnp.float32)
    vf = v.astype(jnp.float32)
    scale = 1.0 / math.sqrt(DH)

    def blk(qp):
        qq, pp = qp
        s = jnp.einsum('qkgd,skd->kgqs', qq.astype(jnp.float32), kf) * scale
        s = jnp.where(p[None, None, None, :] <= pp[None, None, :, None], s, -1e30)
        e = jnp.exp(s - jnp.max(s, axis=-1, keepdims=True))
        w = (e / jnp.sum(e, axis=-1, keepdims=True)).astype(jnp.bfloat16)
        o = jnp.einsum('kgqs,skd->qkgd', w.astype(jnp.float32), vf)
        return o.astype(jnp.bfloat16)

    return lax.map(blk, (qr, pr)).reshape(T, HQ * DH)


def reference(x, pos, g1, g2, wq, wk, wv, wo, w1, w3, w2):
    a = rms_norm(x, g1)
    q = rope(jnp.dot(a, wq, preferred_element_type=jnp.float32).reshape(T, HQ, DH), pos).astype(jnp.bfloat16)
    k = rope(jnp.dot(a, wk, preferred_element_type=jnp.float32).reshape(T, HKV, DH), pos).astype(jnp.bfloat16)
    v = jnp.dot(a, wv, preferred_element_type=jnp.float32).astype(jnp.bfloat16).reshape(T, HKV, DH)
    o = attention(q, k, v, pos)
    h1 = (x.astype(jnp.float32) + jnp.dot(o, wo, preferred_element_type=jnp.float32)).astype(jnp.bfloat16)
    b = rms_norm(h1, g2)
    hid = (jax.nn.silu(jnp.dot(b, w1, preferred_element_type=jnp.float32)) * jnp.dot(b, w3, preferred_element_type=jnp.float32)).astype(jnp.bfloat16)
    return (h1.astype(jnp.float32) + jnp.dot(hid, w2, preferred_element_type=jnp.float32)).astype(jnp.bfloat16)
```

```python
import functools
import math
import jax
import jax.numpy as jnp
from jax import lax
from jax.experimental import pallas as pl
from jax.experimental.pallas import tpu as pltpu
from jax.sharding import PartitionSpec as P

DH = 128
EPS = 1e-5
THETA = 500000.0
NEG = -1e30
LC = math.log2(math.e) / math.sqrt(DH)
PC = 512
GRP = 6


def rms_norm(v, g):
    vf = v.astype(jnp.float32)
    inv = lax.rsqrt(jnp.mean(vf * vf, axis=-1, keepdims=True) + EPS)
    return (vf * inv * g.astype(jnp.float32)).astype(jnp.bfloat16)


def rope(y, c, s):
    half = DH // 2
    y1 = y[..., :half]
    y2 = y[..., half:]
    return jnp.concatenate([y1 * c - y2 * s, y2 * c + y1 * s], axis=-1)


def attn_kernel(nsrc, masked, first, last, tab, *refs):
    refs = list(refs)
    q_ref = refs.pop(0)
    k_refs = [refs.pop(0) for _ in range(nsrc)]
    v_refs = [refs.pop(0) for _ in range(nsrc)]
    if not first:
        ai_ref = refs.pop(0)
        mi_ref = refs.pop(0)
    if last:
        o_ref = refs.pop(0)
    else:
        ao_ref = refs.pop(0)
        mo_ref = refs.pop(0)
    m_s, al_s, acc_s, ks, vs, s0, s1, p0, p1 = refs
    S = [s0, s1]
    PP = [p0, p1]
    units = 2 * nsrc + (1 if masked else 0)
    for i in range(nsrc):
        ks[i * 1024:(i + 1) * 1024, :] = k_refs[i][...]
        vs[i * 1024:(i + 1) * 1024, :] = v_refs[i][...]
    if first:
        m_s[...] = jnp.full_like(m_s, NEG)
        acc_s[...] = jnp.zeros_like(acc_s)
    else:
        for qp in range(2):
            for h in range(GRP):
                m_s[qp, h] = jnp.broadcast_to(mi_ref[qp, :, h:h + 1], (PC, 128))
                acc_s[qp, h, :, :128] = ai_ref[qp, h]
                acc_s[qp, h, :, 128:] = jnp.broadcast_to(mi_ref[qp, :, 64 + h:65 + h], (PC, 128))
    al_s[...] = jnp.ones_like(al_s)
    p1[...] = jnp.zeros_like(p1)
    ones = jnp.ones((PC, 128), jnp.bfloat16)

    def qk(u, h):
        qo = pl.multiple_of(tab[u, 0] * PC, PC)
        ko = pl.multiple_of(tab[u, 1] * PC, PC)
        S[h % 2][...] = lax.dot_general(q_ref[pl.ds(qo, PC), h * 128:(h + 1) * 128], ks[pl.ds(ko, PC), :],
                                        (((1,), (1,)), ((), ())), preferred_element_type=jnp.float32)

    def sm(u, h):
        qp = tab[u, 0]
        s = S[h % 2][...]
        if masked:
            r = lax.broadcasted_iota(jnp.int32, s.shape, 0)
            c = lax.broadcasted_iota(jnp.int32, s.shape, 1)
            s = jnp.where(c - r <= tab[u, 2], s, NEG)
        mx = jnp.max(s, axis=1, keepdims=True)
        mp = m_s[qp, h]
        mn = jnp.maximum(mp, mx)
        al_s[h % 2] = jnp.exp2((mp - mn) * LC)
        pr = jnp.exp2(s * LC - jnp.tile(mn * LC, (1, PC // 128)))
        PP[h % 2][...] = pr.astype(jnp.bfloat16)
        m_s[qp, h] = mn

    def pv(u, h):
        qp = tab[u, 0]
        ko = pl.multiple_of(tab[u, 1] * PC, PC)
        vb = jnp.concatenate([vs[pl.ds(ko, PC), :], ones], axis=1)
        x = jnp.dot(PP[h % 2][...], vb, preferred_element_type=jnp.float32)
        acc_s[qp, h] = acc_s[qp, h] * jnp.tile(al_s[h % 2], (1, 2)) + x

    qk(0, 0)

    def body(u, _):
        for h in range(GRP):
            qk(u if h < GRP - 1 else jnp.minimum(u + 1, units - 1), (h + 1) % GRP)
            pv(jnp.maximum(u - 1, 0) if h == 0 else u, (h - 1) % GRP)
            sm(u, h)
        return 0

    lax.fori_loop(0, units, body, 0)
    pv(units - 1, GRP - 1)
    if last:
        for qp in range(2):
            for h in range(GRP):
                a = acc_s[qp, h]
                o_ref[qp * PC:(qp + 1) * PC, h * 128:(h + 1) * 128] = (a[:, :128] / a[:, 128:]).astype(jnp.bfloat16)
    else:
        lane = lax.broadcasted_iota(jnp.int32, (PC, 128), 1)
        for qp in range(2):
            ml = jnp.zeros((PC, 128), jnp.float32)
            for h in range(GRP):
                ao_ref[qp, h] = acc_s[qp, h, :, :128]
                ml = jnp.where(lane == h, m_s[qp, h], ml)
                ml = jnp.where(lane == 64 + h, acc_s[qp, h, :, 128:], ml)
            mo_ref[qp] = ml


def attn_call(tab, q, ks, vs, state, masked, last, name):
    nsrc = len(ks)
    first = state is None
    qs = pl.BlockSpec((1024, 768), lambda g, t: (0, g))
    kv = pl.BlockSpec((1024, 128), lambda g, t: (0, g))
    sa = pl.BlockSpec((None, 2, GRP, PC, 128), lambda g, t: (g, 0, 0, 0, 0))
    sml = pl.BlockSpec((None, 2, PC, 128), lambda g, t: (g, 0, 0, 0))
    ins = [qs] + [kv] * (2 * nsrc) + ([] if first else [sa, sml])
    if last:
        outs = qs
        osh = jax.ShapeDtypeStruct((1024, 1536), jnp.bfloat16)
    else:
        outs = [sa, sml]
        osh = [jax.ShapeDtypeStruct((2, 2, GRP, PC, 128), jnp.float32), jax.ShapeDtypeStruct((2, 2, PC, 128), jnp.float32)]
    units = 2 * nsrc + (1 if masked else 0)
    return pl.pallas_call(
        functools.partial(attn_kernel, nsrc, masked, first, last),
        grid_spec=pltpu.PrefetchScalarGridSpec(
            num_scalar_prefetch=1, grid=(2,), in_specs=ins, out_specs=outs,
            scratch_shapes=[
                pltpu.VMEM((2, GRP, PC, 128), jnp.float32), pltpu.VMEM((2, PC, 128), jnp.float32),
                pltpu.VMEM((2, GRP, PC, 256), jnp.float32),
                pltpu.VMEM((nsrc * 1024, 128), jnp.bfloat16), pltpu.VMEM((nsrc * 1024, 128), jnp.bfloat16),
                pltpu.VMEM((PC, PC), jnp.float32), pltpu.VMEM((PC, PC), jnp.float32),
                pltpu.VMEM((PC, PC), jnp.bfloat16), pltpu.VMEM((PC, PC), jnp.bfloat16)]),
        out_shape=osh,
        compiler_params=pltpu.CompilerParams(vmem_limit_bytes=60 * 2**20),
        cost_estimate=pl.CostEstimate(flops=units * 12 * 2 * PC * PC * 512, bytes_accessed=20 * 2**20, transcendentals=units * 12 * PC * PC),
        name=name)(tab, q, *ks, *vs, *([] if first else state))


def solution(mesh):
    tok = P(('dp', 'cp', 'tp'), None)
    col = P(None, 'tp')
    row = P('tp', None)
    ncp = mesh.shape['cp']
    ntp = mesh.shape['tp']

    def perm(v, dc, dj):
        pairs = []
        for c in range(ncp):
            for j in range(ntp):
                pairs.append((j * ncp + c, (j ^ dj) * ncp + (c ^ dc)))
        return lax.ppermute(v, ('tp', 'cp'), pairs)

    def local(x, pos, g1, g2, wq, wk, wv, wo, w1, w3, w2):
        c = lax.axis_index('cp')
        j = lax.axis_index('tp')
        k = c * ntp + j
        core = c % 2

        def other_half(w):
            n = w.shape[0] // 2
            mine = lax.dynamic_slice_in_dim(w, core * n, n, 0)
            got = perm(mine, 0, 1)
            sib = perm(got, 1, 0)
            return jnp.where(core == 0, jnp.concatenate([got, sib], 0), jnp.concatenate([sib, got], 0))

        wkv = jnp.concatenate([wk, wv], 1)
        wkv_o = other_half(wkv)
        wq_o = other_half(wq)
        wo_o = other_half(wo)

        a = rms_norm(x, g1)
        freq = 1.0 / (THETA ** (jnp.arange(0, DH, 2, dtype=jnp.float32) / DH))
        ang = pos.astype(jnp.float32)[:, None] * freq
        cs = jnp.cos(ang)[:, None, :]
        sn = jnp.sin(ang)[:, None, :]

        def proj(w):
            return jnp.dot(a, w, preferred_element_type=jnp.float32)

        def swap(m, o, ax=1):
            return jnp.where(j == 0, jnp.concatenate([m, o], ax), jnp.concatenate([o, m], ax))

        kvm = proj(wkv)
        kvo = proj(wkv_o)

        def kpart(y):
            return rope(y[:, :DH].reshape(1024, 1, DH), cs, sn).astype(jnp.bfloat16).reshape(1024, DH)

        kk = swap(kpart(kvm), kpart(kvo))
        vv = swap(kvm[:, DH:].astype(jnp.bfloat16), kvo[:, DH:].astype(jnp.bfloat16))
        kva = jnp.concatenate([kk, vv], 1)
        kvs = perm(kva, 1, 0)
        kvx = perm(kva, 2, 0)
        kvy = perm(kva, 0, 1)
        kvxs = perm(kvx, 1, 0)
        kvys = perm(kvy, 1, 0)
        z1 = perm(kvx[:512], 0, 1)
        z2 = perm(kvy[512:], 2, 0)
        kvz = jnp.concatenate([z1, z2], 0)
        kvzs = perm(kvz, 1, 0)

        def qpart(w):
            return rope(proj(w).reshape(1024, GRP, DH), cs, sn).astype(jnp.bfloat16).reshape(1024, GRP * DH)

        q = swap(qpart(wq), qpart(wq_o))

        def units(devs, base):
            rows = []
            for i, d in enumerate(devs):
                gt = d > k
                rows.append(jnp.stack([jnp.where(gt, 1, 0), jnp.int32(2 * (i + base)), jnp.int32(PC)]))
                rows.append(jnp.stack([jnp.int32(1), jnp.where(gt, 2 * (i + base) + 1, 2 * (i + base)), jnp.int32(PC)]))
            return rows

        def dev(dc, dj):
            return (c ^ dc) * ntp + (j ^ dj)

        t1 = jnp.stack([jnp.array([0, 0, 0], jnp.int32), jnp.array([1, 1, 0], jnp.int32), jnp.array([1, 0, PC], jnp.int32)]
                       + units([dev(1, 0)], 1)).astype(jnp.int32)
        t2 = jnp.stack(units([dev(2, 0), dev(3, 0), dev(0, 1), dev(1, 1)], 0)).astype(jnp.int32)
        t3 = jnp.stack(units([dev(2, 1), dev(3, 1)], 0)).astype(jnp.int32)
        sp = lambda t: (t[:, :256], t[:, 256:])
        st = attn_call(t1, q, *zip(*map(sp, [kva, kvs])), None, True, False, "attn1")
        st = attn_call(t2, q, *zip(*map(sp, [kvx, kvxs, kvy, kvys])), st, False, False, "attn2")
        o = attn_call(t3, q, *zip(*map(sp, [kvz, kvzs])), st, False, True, "attn3")

        wof = swap(wo, wo_o, 0)
        h1 = (x.astype(jnp.float32) + jnp.dot(o, wof, preferred_element_type=jnp.float32)).astype(jnp.bfloat16)
        hp = [perm(h1[:512], 0, 1), perm(h1[512:], 0, 1)]

        def mlp(h):
            b = rms_norm(h, g2)
            hid = (jax.nn.silu(jnp.dot(b, w1, preferred_element_type=jnp.float32)) * jnp.dot(b, w3, preferred_element_type=jnp.float32)).astype(jnp.bfloat16)
            return jnp.dot(hid, w2, preferred_element_type=jnp.float32)

        zp = [perm(mlp(h).astype(jnp.bfloat16), 0, 1) for h in hp]
        z = mlp(h1)
        zr = jnp.concatenate(zp, 0).astype(jnp.float32)
        return (h1.astype(jnp.float32) + (z + zr)).astype(jnp.bfloat16)

    return jax.shard_map(local, mesh=mesh, in_specs=(tok, P(('dp', 'cp', 'tp')), P(None), P(None), col, col, col, row, col, col, row), out_specs=tok, check_vma=False)
```

```python
import functools
import math
import jax
import jax.numpy as jnp
import numpy as np
from jax import lax
from jax.experimental import pallas as pl
from jax.experimental.pallas import tpu as pltpu
from jax.sharding import PartitionSpec as P

DH = 128
EPS = 1e-5
THETA = 500000.0
NEG = -1e30
LC = math.log2(math.e) / math.sqrt(DH)
PC = 512
GRP = 6
D = 1536
QW = GRP * DH
FT = 896
VM = 62 * 2**20
MESH = pl.DeviceIdType.MESH


def cparams():
    return pltpu.CompilerParams(vmem_limit_bytes=VM)


def cost(flops, byts, tr=0):
    return pl.CostEstimate(flops=int(flops), bytes_accessed=int(byts), transcendentals=int(tr))


def rms(v, g):
    vf = v.astype(jnp.float32)
    inv = lax.rsqrt(jnp.mean(vf * vf, axis=-1, keepdims=True) + EPS)
    return (vf * inv * g.astype(jnp.float32)).astype(jnp.bfloat16)


def att_kernel(x_h, g_ref, cs_h, sn_h, wq_h, wk_h, wv_h, wo_h,
               h_ref, hp_ref,
               xv, csv, snv, wqb, wkb, wvb, wob, qb, kvb, m_s, al_s, acc_s, s0, s1, p0, p1, ob, hs,
               ld, ks, kr, ws, wr, hsem):
    c = lax.axis_index('cp')
    j = lax.axis_index('tp')
    core = lax.rem(c, 2)
    k = c * 2 + j
    cs_ = c + 1 - 2 * core
    cx = lax.rem(c + 2, 4)
    cxs = lax.rem(cs_ + 2, 4)
    SIB = {"cp": cs_}
    XP = {"cp": cx}
    YP = {"tp": 1 - j}
    S = [s0, s1]
    PP = [p0, p1]

    def rc(src, dst, ss, rs, dev):
        return pltpu.make_async_remote_copy(src_ref=src, dst_ref=dst, send_sem=ss, recv_sem=rs, device_id=dev, device_id_type=MESH)

    loads = [(x_h, xv), (wq_h, wqb.at[0]), (wk_h, wkb.at[0]), (wv_h, wvb.at[0]), (cs_h, csv), (sn_h, snv)]
    loads = [pltpu.make_async_copy(a, b, ld.at[i]) for i, (a, b) in enumerate(loads)]
    wol = pltpu.make_async_copy(wo_h, wob.at[pl.ds(0, QW)], ld.at[6])
    for l in loads:
        l.start()

    bar = pltpu.get_barrier_semaphore()
    for d in (SIB, XP, YP):
        pl.semaphore_signal(bar, inc=1, device_id=d, device_id_type=MESH)
    pl.semaphore_wait(bar, 3)

    wsrc = [wk_h, wv_h, wq_h, wo_h]
    wdst = [wkb.at[1], wvb.at[1], wqb.at[1], wob.at[pl.ds(QW, QW)]]

    def wcopy(i, hop):
        n = wsrc[i].shape[0] // 4
        q = c if hop < 3 else cx
        o = pl.multiple_of(q * n, n)
        dst = wdst[i].at[pl.ds(o, n)]
        src = wsrc[i].at[pl.ds(o, n)] if hop == 0 else dst
        return rc(src, dst, ws.at[i, hop], wr.at[i, hop], (YP, SIB, XP, SIB)[hop])

    def wrecv(i, hop):
        n = wsrc[i].shape[0] // 4
        q = (c, cs_, cx, cxs)[hop]
        dst = wdst[i].at[pl.ds(pl.multiple_of(q * n, n), n)]
        rc(dst, dst, ws.at[i, hop], wr.at[i, hop], (YP, SIB, XP, SIB)[hop]).wait_recv()

    KV = {'S': (0, 0, 0, 2, SIB), 'X': (0, 0, 0, 4, XP), 'Y': (0, 0, 1, 1, YP), 'XS': (0, 4, 0, 6, SIB),
          'YS': (1, 1, 1, 3, SIB), 'Z': (1, 1, 1, 5, XP), 'ZS': (1, 5, 1, 7, SIB),
          's': (1, 0, 1, 2, SIB), 'x': (1, 0, 1, 4, XP), 'y': (1, 0, 0, 1, YP), 'xs': (1, 4, 1, 6, SIB),
          'ys': (0, 1, 0, 3, SIB), 'z': (0, 1, 0, 5, XP), 'zs': (0, 5, 0, 7, SIB)}

    def kcopy(n):
        gs, ms, gd, md, dev = KV[n]
        return rc(kvb.at[gs, ms], kvb.at[gd, md], ks.at[gd, md], kr.at[gd, md], dev)

    for i in range(3):
        wcopy(i, 0).start()
    for l in loads:
        l.wait()
    wol.start()

    def front(g):
        def blk(i, _):
            r = pl.ds(pl.multiple_of(i * 256, 256), 256)
            a = rms(xv[r, :], g_ref[...])
            w = jnp.concatenate([wqb[g], wkb[g], wvb[g]], axis=1)
            y = jnp.dot(a, w, preferred_element_type=jnp.float32)
            cc = csv[r, :]
            sc = snv[r, :]
            for h in range(GRP + 1):
                u = y[:, h * DH:(h + 1) * DH]
                v = (u * cc + pltpu.roll(u, DH // 2, 1) * sc).astype(jnp.bfloat16)
                if h < GRP:
                    qb[g, r, h * DH:(h + 1) * DH] = v
                else:
                    kvb[g, 0, r, :DH] = v
            kvb[g, 0, r, DH:] = y[:, QW + DH:].astype(jnp.bfloat16)
            return 0

        lax.fori_loop(0, 4, blk, 0)

    front(0)
    for n in 'SXY':
        kcopy(n).start()

    m_s[...] = jnp.full_like(m_s, NEG)
    acc_s[...] = jnp.zeros_like(acc_s)
    al_s[...] = jnp.ones_like(al_s)
    p1[...] = jnp.zeros_like(p1)
    ones = jnp.ones((PC, 128), jnp.bfloat16)

    two = lambda g, ms: [(g, m, t) for m in ms for t in (3, 4)]
    own = lambda g: [(g, 0, 0), (g, 0, 1), (g, 0, 2)]
    last8 = [(1, 4), (1, 6), (0, 1), (0, 3), (1, 5), (1, 7), (0, 5), (0, 7)]
    seq = own(0) + two(0, (2, 4, 6)) + own(1) + two(1, (2, 1, 3)) + [(g, m, 3) for g, m in last8] + [(g, m, 4) for g, m in last8]
    NU = len(seq)
    codes = [g * 64 + m * 8 + t for g, m, t in seq]

    def code_of(u):
        v = jnp.int32(codes[0])
        for i in range(1, NU):
            v = jnp.where(u == i, codes[i], v)
        return v

    def decode(cd):
        g = cd // 64
        m = (cd // 8) % 8
        t = cd % 8
        lt = jnp.where(m >= 4, k // 4, jnp.where(m >= 2, (k // 2) % 2, k % 2))
        qp = jnp.where(t == 0, 0, jnp.where(t == 3, 1 - lt, 1))
        hf = jnp.where(t == 1, 1, jnp.where(t == 4, 1 - lt, 0))
        return g, m, t, qp, hf

    def qk(e, h):
        g, m, t, qp, hf = e
        qo = pl.multiple_of(qp * PC, PC)
        ko = pl.multiple_of(hf * PC, PC)
        S[h % 2][...] = lax.dot_general(qb[g, pl.ds(qo, PC), h * DH:(h + 1) * DH], kvb[g, m, pl.ds(ko, PC), :DH],
                                        (((1,), (1,)), ((), ())), preferred_element_type=jnp.float32)

    def sm(e, h, masked):
        g, m, t, qp, hf = e
        s = S[h % 2][...]
        if masked:
            r = lax.broadcasted_iota(jnp.int32, s.shape, 0)
            cc = lax.broadcasted_iota(jnp.int32, s.shape, 1)
            s = jnp.where(cc <= r, s, NEG)
        mx = jnp.max(s, axis=1, keepdims=True)
        mp = m_s[g, qp, h]
        mn = jnp.maximum(mp, mx)
        al_s[h % 2] = jnp.exp2((mp - mn) * LC)
        pr = jnp.exp2(s * LC - jnp.tile(mn * LC, (1, PC // 128)))
        PP[h % 2][...] = pr.astype(jnp.bfloat16)
        m_s[g, qp, h] = mn

    def pv(e, h):
        g, m, t, qp, hf = e
        ko = pl.multiple_of(hf * PC, PC)
        vb = jnp.concatenate([kvb[g, m, pl.ds(ko, PC), DH:], ones], axis=1)
        y = jnp.dot(PP[h % 2][...], vb, preferred_element_type=jnp.float32)
        acc_s[g, qp, h] = acc_s[g, qp, h] * jnp.tile(al_s[h % 2], (1, 2)) + y

    def finalize(qp):
        for g in range(2):
            for h in range(GRP):
                a = acc_s[g, qp, h]
                ob[:, (g * GRP + h) * DH:(g * GRP + h + 1) * DH] = (a[:, :128] / a[:, 128:]).astype(jnp.bfloat16)

        def blk(i, _):
            r = pl.ds(pl.multiple_of(i * 256, 256), 256)
            rx = pl.ds(pl.multiple_of(qp * PC + i * 256, 256), 256)
            y = jnp.dot(ob[r, :], wob[...], preferred_element_type=jnp.float32)
            hs[rx, :] = (xv[rx, :].astype(jnp.float32) + y).astype(jnp.bfloat16)
            return 0

        lax.fori_loop(0, 2, blk, 0)

    hcopy = rc(hs.at[pl.ds(0, PC)], hp_ref, hsem.at[0], hsem.at[1], YP)
    hout = [pltpu.make_async_copy(hs.at[pl.ds(i * PC, PC)], h_ref.at[pl.ds(i * PC, PC)], ld.at[7 + i]) for i in range(2)]

    kw = lambda n: kcopy(n).wait_recv()

    def act(u):
        def at(i):
            return pl.when(u == i)

        @at(2)
        def _():
            kw('S')

        @at(4)
        def _():
            kw('X')
            kcopy('XS').start()
            for i in range(3):
                wrecv(i, 0)
            for i in range(3):
                wcopy(i, 2).start()
                wcopy(i, 1).start()
            wcopy(3, 0).start()

        @at(6)
        def _():
            kw('XS')

        @at(8)
        def _():
            kw('Y')
            kcopy('YS').start()
            for i in range(3):
                wrecv(i, 2)
                wcopy(i, 3).start()
            kcopy('Z').start()
            for i in range(3):
                wrecv(i, 1)
            for i in range(3):
                wrecv(i, 3)
            front(1)
            for n in 'sxy':
                kcopy(n).start()

        @at(11)
        def _():
            kw('s')

        @at(13)
        def _():
            wrecv(3, 0)
            wcopy(3, 1).start()

        @at(15)
        def _():
            kw('YS')

        @at(16)
        def _():
            kw('y')
            kcopy('ys').start()
            kcopy('z').start()
            wcopy(3, 2).start()

        @at(17)
        def _():
            kw('x')
            kcopy('xs').start()
            kw('Z')
            kcopy('ZS').start()

        @at(18)
        def _():
            kw('xs')

        @at(20)
        def _():
            kw('ys')

        @at(22)
        def _():
            kw('ZS')

        @at(23)
        def _():
            kw('z')
            kcopy('zs').start()

        @at(24)
        def _():
            kw('zs')

        @at(26)
        def _():
            wrecv(3, 2)
            wcopy(3, 3).start()

        @at(27)
        def _():
            wol.wait()
            wrecv(3, 1)
            wrecv(3, 3)
            finalize(0)
            hcopy.start()
            hout[0].start()

    e0 = decode(jnp.int32(codes[0]))
    qk(e0, 0)

    def body(u, carry):
        cc, pc = carry
        act(u)
        nc = code_of(jnp.minimum(u + 1, NU - 1))
        cur, prv, nxt = decode(cc), decode(pc), decode(nc)

        def run(masked):
            for h in range(GRP):
                if h < GRP - 1:
                    qk(cur, h + 1)
                else:
                    qk(nxt, 0)
                if h == 0:
                    pv(prv, GRP - 1)
                else:
                    pv(cur, h - 1)
                sm(cur, h, masked)

        diag = cur[2] < 2

        @pl.when(diag)
        def _():
            run(True)

        @pl.when(jnp.logical_not(diag))
        def _():
            run(False)

        return nc, cc

    fin = lax.fori_loop(0, NU, body, (jnp.int32(codes[0]), jnp.int32(codes[0])))
    pv(decode(fin[1]), GRP - 1)
    finalize(1)
    hout[1].start()
    hcopy.wait_recv()
    hcopy.wait_send()
    for o in hout:
        o.wait()
    for n in KV:
        kcopy(n).wait_send()
    for i in range(4):
        for hop in range(4):
            wcopy(i, hop).wait_send()


def att(x, g, cs, sn, wq, wk, wv, wo):
    n = x.shape[0]
    any_ = pl.BlockSpec(memory_space=pl.ANY)
    vm = pl.BlockSpec(memory_space=pltpu.VMEM)
    bf, f32 = jnp.bfloat16, jnp.float32
    return pl.pallas_call(
        att_kernel,
        in_specs=[any_, vm] + [any_] * 6,
        out_specs=[any_, any_],
        out_shape=[jax.ShapeDtypeStruct((n, D), bf), jax.ShapeDtypeStruct((PC, D), bf)],
        scratch_shapes=[
            pltpu.VMEM((n, D), bf), pltpu.VMEM((n, DH), f32), pltpu.VMEM((n, DH), f32),
            pltpu.VMEM((2, D, QW), bf), pltpu.VMEM((2, D, DH), bf), pltpu.VMEM((2, D, DH), bf), pltpu.VMEM((D, D), bf),
            pltpu.VMEM((2, n, QW), bf), pltpu.VMEM((2, 8, n, 2 * DH), bf),
            pltpu.VMEM((2, 2, GRP, PC, 128), f32), pltpu.VMEM((2, PC, 128), f32), pltpu.VMEM((2, 2, GRP, PC, 256), f32),
            pltpu.VMEM((PC, PC), f32), pltpu.VMEM((PC, PC), f32), pltpu.VMEM((PC, PC), bf), pltpu.VMEM((PC, PC), bf),
            pltpu.VMEM((PC, D), bf), pltpu.VMEM((n, D), bf),
            pltpu.SemaphoreType.DMA((9,)), pltpu.SemaphoreType.DMA((2, 8)), pltpu.SemaphoreType.DMA((2, 8)),
            pltpu.SemaphoreType.DMA((4, 4)), pltpu.SemaphoreType.DMA((4, 4)), pltpu.SemaphoreType.DMA((2,))],
        compiler_params=pltpu.CompilerParams(collective_id=0, has_side_effects=True, vmem_limit_bytes=VM),
        cost_estimate=cost(70e9, 20 * 2**20), name="att")(x, g, cs, sn, wq, wk, wv, wo)


def mlp_kernel(n1, h_ref, g_ref, w1_ref, w3_ref, w2_ref, o_ref, b_s, hid_s):
    i = pl.program_id(0)

    @pl.when(i == 0)
    def _():
        b_s[...] = rms(h_ref[...], g_ref[...])

    @pl.when(i < n1)
    def _():
        w = jnp.concatenate([w1_ref[...], w3_ref[...]], axis=1)
        y = jnp.dot(b_s[...], w, preferred_element_type=jnp.float32)
        a = y[:, :FT]
        hid_s[i] = (a * jax.nn.sigmoid(a) * y[:, FT:]).astype(jnp.bfloat16)

    @pl.when(i >= n1)
    def _():
        hid = jnp.concatenate([hid_s[t] for t in range(n1)], axis=1)
        o_ref[...] = jnp.dot(hid, w2_ref[...], preferred_element_type=jnp.float32).astype(o_ref.dtype)


def mlp(h, g, w1, w3, w2, dt, name):
    n = h.shape[0]
    f = w1.shape[1]
    n1 = f // FT
    n2 = 3
    wn = D // n2
    up = pl.BlockSpec((D, FT), lambda i: (0, jnp.minimum(i, n1 - 1)))
    dn = lambda r: pl.BlockSpec((r, wn), lambda i: (0, jnp.maximum(i - n1, 0)))
    return pl.pallas_call(
        functools.partial(mlp_kernel, n1), grid=(n1 + n2,),
        in_specs=[pl.BlockSpec((n, D), lambda i: (0, 0)), pl.BlockSpec((1, D), lambda i: (0, 0)), up, up, dn(f)],
        out_specs=dn(n),
        scratch_shapes=[pltpu.VMEM((n, D), jnp.bfloat16), pltpu.VMEM((n1, n, FT), jnp.bfloat16)],
        out_shape=jax.ShapeDtypeStruct((n, D), dt),
        compiler_params=cparams(), cost_estimate=cost(6 * n * D * f, 6 * D * f), name=name)(h, g, w1, w3, w2)


def solution(mesh):
    tok = P(('dp', 'cp', 'tp'), None)
    col = P(None, 'tp')
    row = P('tp', None)
    ncp = mesh.shape['cp']
    ntp = mesh.shape['tp']

    def perm(v, dc, dj):
        pairs = []
        for c in range(ncp):
            for j in range(ntp):
                pairs.append((j * ncp + c, (j ^ dj) * ncp + (c ^ dc)))
        return lax.ppermute(v, ('tp', 'cp'), pairs)

    def local(x, pos, g1, g2, wq, wk, wv, wo, w1, w3, w2):
        freq = 1.0 / (THETA ** (jnp.arange(0, DH, 2, dtype=jnp.float32) / DH))
        ang = pos.astype(jnp.float32)[:, None] * freq
        cs = jnp.cos(ang)
        sn = jnp.sin(ang)
        cs = jnp.concatenate([cs, cs], 1)
        sn = jnp.concatenate([-sn, sn], 1)
        g2r = g2.reshape(1, D)
        h, hp_b = att(x, g1.reshape(1, D), cs, sn, wq, wk, wv, wo)
        h_b = h[:PC]
        h_a = h[PC:]
        hp_a = perm(h_a, 0, 1)
        z_b = perm(mlp(hp_b, g2r, w1, w3, w2, jnp.bfloat16, "mlp_pb"), 0, 1)
        z_a = perm(mlp(hp_a, g2r, w1, w3, w2, jnp.bfloat16, "mlp_pa"), 0, 1)
        out = []
        for hh, zr, nm in ((h_b, z_b, "mlp_ob"), (h_a, z_a, "mlp_oa")):
            z = mlp(hh, g2r, w1, w3, w2, jnp.float32, nm)
            out.append((hh.astype(jnp.float32) + (z + zr.astype(jnp.float32))).astype(jnp.bfloat16))
        return jnp.concatenate(out, 0)

    return jax.shard_map(local, mesh=mesh, in_specs=(tok, P(('dp', 'cp', 'tp')), P(None), P(None), col, col, col, row, col, col, row), out_specs=tok, check_vma=False)
```

```python
import functools
import math
import jax
import jax.numpy as jnp
from jax import lax
from jax.experimental import pallas as pl
from jax.experimental.pallas import tpu as pltpu
from jax.sharding import PartitionSpec as P

DH = 128
EPS = 1e-5
THETA = 500000.0
NEG = -1e30
LC = math.log2(math.e) / math.sqrt(DH)
PC = 512
GRP = 6
D = 1536
QW = GRP * DH
VM = 62 * 2**20
MESH = pl.DeviceIdType.MESH


def cost(flops, byts, tr=0):
    return pl.CostEstimate(flops=int(flops), bytes_accessed=int(byts), transcendentals=int(tr))


def rms(v, g):
    vf = v.astype(jnp.float32)
    inv = lax.rsqrt(jnp.mean(vf * vf, axis=-1, keepdims=True) + EPS)
    return (vf * inv * g.astype(jnp.float32)).astype(jnp.bfloat16)


def att_kernel(x_h, g_ref, cs_h, sn_h, wq_h, wk_h, wv_h, wo_h,
               h_ref, hp_ref,
               xv, csv, snv, wqb, wkb, wvb, wob, qb, kvb, m_s, al_s, acc_s, s0, s1, p0, p1, ob, hs,
               ld, ks, kr, ws, wr, hsem):
    c = lax.axis_index('cp')
    j = lax.axis_index('tp')
    core = lax.rem(c, 2)
    k = c * 2 + j
    cs_ = c + 1 - 2 * core
    cx = lax.rem(c + 2, 4)
    cxs = lax.rem(cs_ + 2, 4)
    SIB = {"cp": cs_}
    XP = {"cp": cx}
    YP = {"tp": 1 - j}
    S = [s0, s1]
    PP = [p0, p1]

    def rc(src, dst, ss, rs, dev):
        return pltpu.make_async_remote_copy(src_ref=src, dst_ref=dst, send_sem=ss, recv_sem=rs, device_id=dev, device_id_type=MESH)

    loads = [(x_h, xv), (wq_h, wqb.at[0]), (wk_h, wkb.at[0]), (wv_h, wvb.at[0]), (cs_h, csv), (sn_h, snv)]
    loads = [pltpu.make_async_copy(a, b, ld.at[i]) for i, (a, b) in enumerate(loads)]
    wol = pltpu.make_async_copy(wo_h, wob.at[pl.ds(0, QW)], ld.at[6])
    for l in loads:
        l.start()

    bar = pltpu.get_barrier_semaphore()
    for d in (SIB, XP, YP):
        pl.semaphore_signal(bar, inc=1, device_id=d, device_id_type=MESH)
    pl.semaphore_wait(bar, 3)

    wsrc = [wk_h, wv_h, wq_h, wo_h]
    wdst = [wkb.at[1], wvb.at[1], wqb.at[1], wob.at[pl.ds(QW, QW)]]

    def wcopy(i, hop):
        n = wsrc[i].shape[0] // 4
        q = c if hop < 3 else cx
        o = pl.multiple_of(q * n, n)
        dst = wdst[i].at[pl.ds(o, n)]
        src = wsrc[i].at[pl.ds(o, n)] if hop == 0 else dst
        return rc(src, dst, ws.at[i, hop], wr.at[i, hop], (YP, SIB, XP, SIB)[hop])

    def wrecv(i, hop):
        n = wsrc[i].shape[0] // 4
        q = (c, cs_, cx, cxs)[hop]
        dst = wdst[i].at[pl.ds(pl.multiple_of(q * n, n), n)]
        rc(dst, dst, ws.at[i, hop], wr.at[i, hop], (YP, SIB, XP, SIB)[hop]).wait_recv()

    KV = {'S': (0, 0, 0, 2, SIB), 'X': (0, 0, 0, 4, XP), 'Y': (0, 0, 1, 1, YP), 'XS': (0, 4, 0, 6, SIB),
          'YS': (1, 1, 1, 3, SIB), 'Z': (1, 1, 1, 5, XP), 'ZS': (1, 5, 1, 7, SIB),
          's': (1, 0, 1, 2, SIB), 'x': (1, 0, 1, 4, XP), 'y': (1, 0, 0, 1, YP), 'xs': (1, 4, 1, 6, SIB),
          'ys': (0, 1, 0, 3, SIB), 'z': (0, 1, 0, 5, XP), 'zs': (0, 5, 0, 7, SIB)}

    def kcopy(n):
        gs, ms, gd, md, dev = KV[n]
        return rc(kvb.at[gs, ms], kvb.at[gd, md], ks.at[gd, md], kr.at[gd, md], dev)

    for i in range(3):
        wcopy(i, 0).start()
    for l in loads:
        l.wait()
    wol.start()

    def front(g):
        def blk(i, _):
            r = pl.ds(pl.multiple_of(i * 256, 256), 256)
            a = rms(xv[r, :], g_ref[...])
            w = jnp.concatenate([wqb[g], wkb[g], wvb[g]], axis=1)
            y = jnp.dot(a, w, preferred_element_type=jnp.float32)
            cc = csv[r, :]
            sc = snv[r, :]
            for h in range(GRP + 1):
                u = y[:, h * DH:(h + 1) * DH]
                v = (u * cc + pltpu.roll(u, DH // 2, 1) * sc).astype(jnp.bfloat16)
                if h < GRP:
                    qb[g, r, h * DH:(h + 1) * DH] = v
                else:
                    kvb[g, 0, r, :DH] = v
            kvb[g, 0, r, DH:] = y[:, QW + DH:].astype(jnp.bfloat16)
            return 0

        lax.fori_loop(0, 4, blk, 0)

    front(0)
    for n in 'SXY':
        kcopy(n).start()

    m_s[...] = jnp.full_like(m_s, NEG)
    acc_s[...] = jnp.zeros_like(acc_s)
    al_s[...] = jnp.ones_like(al_s)
    p1[...] = jnp.zeros_like(p1)
    ones = jnp.ones((PC, 128), jnp.bfloat16)

    two = lambda g, ms: [(g, m, t) for m in ms for t in (3, 4)]
    own = lambda g: [(g, 0, 0), (g, 0, 1), (g, 0, 2)]
    last8 = [(1, 4), (1, 6), (0, 1), (0, 3), (1, 5), (1, 7), (0, 5), (0, 7)]
    seq = own(0) + two(0, (2, 4, 6)) + own(1) + two(1, (2, 1, 3)) + [(g, m, 3) for g, m in last8] + [(g, m, 4) for g, m in last8]
    NU = len(seq)
    codes = [g * 64 + m * 8 + t for g, m, t in seq]

    def code_of(u):
        v = jnp.int32(codes[0])
        for i in range(1, NU):
            v = jnp.where(u == i, codes[i], v)
        return v

    def decode(cd):
        g = cd // 64
        m = (cd // 8) % 8
        t = cd % 8
        lt = jnp.where(m >= 4, k // 4, jnp.where(m >= 2, (k // 2) % 2, k % 2))
        qp = jnp.where(t == 0, 0, jnp.where(t == 3, 1 - lt, 1))
        hf = jnp.where(t == 1, 1, jnp.where(t == 4, 1 - lt, 0))
        return g, m, t, qp, hf

    def qk(e, h):
        g, m, t, qp, hf = e
        qo = pl.multiple_of(qp * PC, PC)
        ko = pl.multiple_of(hf * PC, PC)
        S[h % 2][...] = lax.dot_general(qb[g, pl.ds(qo, PC), h * DH:(h + 1) * DH], kvb[g, m, pl.ds(ko, PC), :DH],
                                        (((1,), (1,)), ((), ())), preferred_element_type=jnp.float32)

    def sm(e, h, masked):
        g, m, t, qp, hf = e
        s = S[h % 2][...]
        if masked:
            r = lax.broadcasted_iota(jnp.int32, s.shape, 0)
            cc = lax.broadcasted_iota(jnp.int32, s.shape, 1)
            s = jnp.where(cc <= r, s, NEG)
        mx = jnp.max(s, axis=1, keepdims=True)
        mp = m_s[g, qp, h]
        mn = jnp.maximum(mp, mx)
        al_s[h % 2] = jnp.exp2((mp - mn) * LC)
        pr = jnp.exp2(s * LC - jnp.tile(mn * LC, (1, PC // 128)))
        PP[h % 2][...] = pr.astype(jnp.bfloat16)
        m_s[g, qp, h] = mn

    def pv(e, h):
        g, m, t, qp, hf = e
        ko = pl.multiple_of(hf * PC, PC)
        vb = jnp.concatenate([kvb[g, m, pl.ds(ko, PC), DH:], ones], axis=1)
        y = jnp.dot(PP[h % 2][...], vb, preferred_element_type=jnp.float32)
        acc_s[g, qp, h] = acc_s[g, qp, h] * jnp.tile(al_s[h % 2], (1, 2)) + y

    def finalize(qp):
        for g in range(2):
            for h in range(GRP):
                a = acc_s[g, qp, h]
                ob[:, (g * GRP + h) * DH:(g * GRP + h + 1) * DH] = (a[:, :128] / a[:, 128:]).astype(jnp.bfloat16)

        def blk(i, _):
            r = pl.ds(pl.multiple_of(i * 256, 256), 256)
            rx = pl.ds(pl.multiple_of(qp * PC + i * 256, 256), 256)
            y = jnp.dot(ob[r, :], wob[...], preferred_element_type=jnp.float32)
            hs[rx, :] = (xv[rx, :].astype(jnp.float32) + y).astype(jnp.bfloat16)
            return 0

        lax.fori_loop(0, 2, blk, 0)

    hcopy = rc(hs.at[pl.ds(0, PC)], hp_ref, hsem.at[0], hsem.at[1], YP)
    hout = [pltpu.make_async_copy(hs.at[pl.ds(i * PC, PC)], h_ref.at[pl.ds(i * PC, PC)], ld.at[7 + i]) for i in range(2)]

    kw = lambda n: kcopy(n).wait_recv()

    def act(u):
        def at(i):
            return pl.when(u == i)

        @at(2)
        def _():
            kw('S')

        @at(4)
        def _():
            kw('X')
            kcopy('XS').start()
            for i in range(3):
                wrecv(i, 0)
            for i in range(3):
                wcopy(i, 2).start()
                wcopy(i, 1).start()
            wcopy(3, 0).start()

        @at(6)
        def _():
            kw('XS')

        @at(8)
        def _():
            kw('Y')
            kcopy('YS').start()
            for i in range(3):
                wrecv(i, 2)
                wcopy(i, 3).start()
            kcopy('Z').start()
            for i in range(3):
                wrecv(i, 1)
            for i in range(3):
                wrecv(i, 3)
            front(1)
            for n in 'sxy':
                kcopy(n).start()

        @at(11)
        def _():
            kw('s')

        @at(13)
        def _():
            wrecv(3, 0)
            wcopy(3, 1).start()

        @at(15)
        def _():
            kw('YS')

        @at(16)
        def _():
            kw('y')
            kcopy('ys').start()
            kcopy('z').start()
            wcopy(3, 2).start()

        @at(17)
        def _():
            kw('x')
            kcopy('xs').start()
            kw('Z')
            kcopy('ZS').start()

        @at(18)
        def _():
            kw('xs')

        @at(20)
        def _():
            kw('ys')

        @at(22)
        def _():
            kw('ZS')

        @at(23)
        def _():
            kw('z')
            kcopy('zs').start()

        @at(24)
        def _():
            kw('zs')

        @at(26)
        def _():
            wrecv(3, 2)
            wcopy(3, 3).start()

        @at(27)
        def _():
            wol.wait()
            wrecv(3, 1)
            wrecv(3, 3)
            finalize(0)
            hcopy.start()
            hout[0].start()

    e0 = decode(jnp.int32(codes[0]))
    qk(e0, 0)

    def body(u, carry):
        cc, pc = carry
        act(u)
        nc = code_of(jnp.minimum(u + 1, NU - 1))
        cur, prv, nxt = decode(cc), decode(pc), decode(nc)

        def run(masked):
            for h in range(GRP):
                if h < GRP - 1:
                    qk(cur, h + 1)
                else:
                    qk(nxt, 0)
                if h == 0:
                    pv(prv, GRP - 1)
                else:
                    pv(cur, h - 1)
                sm(cur, h, masked)

        diag = cur[2] < 2

        @pl.when(diag)
        def _():
            run(True)

        @pl.when(jnp.logical_not(diag))
        def _():
            run(False)

        return nc, cc

    fin = lax.fori_loop(0, NU, body, (jnp.int32(codes[0]), jnp.int32(codes[0])))
    pv(decode(fin[1]), GRP - 1)
    finalize(1)
    hout[1].start()
    hcopy.wait_recv()
    hcopy.wait_send()
    for o in hout:
        o.wait()
    for n in KV:
        kcopy(n).wait_send()
    for i in range(4):
        for hop in range(4):
            wcopy(i, hop).wait_send()


def att(x, g, cs, sn, wq, wk, wv, wo):
    n = x.shape[0]
    any_ = pl.BlockSpec(memory_space=pl.ANY)
    vm = pl.BlockSpec(memory_space=pltpu.VMEM)
    bf, f32 = jnp.bfloat16, jnp.float32
    return pl.pallas_call(
        att_kernel,
        in_specs=[any_, vm] + [any_] * 6,
        out_specs=[any_, any_],
        out_shape=[jax.ShapeDtypeStruct((n, D), bf), jax.ShapeDtypeStruct((PC, D), bf)],
        scratch_shapes=[
            pltpu.VMEM((n, D), bf), pltpu.VMEM((n, DH), f32), pltpu.VMEM((n, DH), f32),
            pltpu.VMEM((2, D, QW), bf), pltpu.VMEM((2, D, DH), bf), pltpu.VMEM((2, D, DH), bf), pltpu.VMEM((D, D), bf),
            pltpu.VMEM((2, n, QW), bf), pltpu.VMEM((2, 8, n, 2 * DH), bf),
            pltpu.VMEM((2, 2, GRP, PC, 128), f32), pltpu.VMEM((2, PC, 128), f32), pltpu.VMEM((2, 2, GRP, PC, 256), f32),
            pltpu.VMEM((PC, PC), f32), pltpu.VMEM((PC, PC), f32), pltpu.VMEM((PC, PC), bf), pltpu.VMEM((PC, PC), bf),
            pltpu.VMEM((PC, D), bf), pltpu.VMEM((n, D), bf),
            pltpu.SemaphoreType.DMA((9,)), pltpu.SemaphoreType.DMA((2, 8)), pltpu.SemaphoreType.DMA((2, 8)),
            pltpu.SemaphoreType.DMA((4, 4)), pltpu.SemaphoreType.DMA((4, 4)), pltpu.SemaphoreType.DMA((2,))],
        compiler_params=pltpu.CompilerParams(collective_id=0, has_side_effects=True, vmem_limit_bytes=VM),
        cost_estimate=cost(70e9, 20 * 2**20), name="att")(x, g, cs, sn, wq, wk, wv, wo)


FU = 640
ND = 512


def mlp_kernel(h_h, hpb_h, g_ref, w1_h, w3_h, w2_h, o_h, hall, wb, w2b, hid, b_s, zs, zr, zo, ld, us, ds, zsem, zrm):
    j = lax.axis_index('tp')
    YP = {"tp": 1 - j}
    F = w1_h.shape[1]
    NU_, NDN = F // FU, D // ND

    def rc(src, dst, ss, rs):
        return pltpu.make_async_remote_copy(src_ref=src, dst_ref=dst, send_sem=ss, recv_sem=rs, device_id=YP, device_id_type=MESH)

    def up(t, slot):
        o = pl.multiple_of(t * FU, 128)
        return [pltpu.make_async_copy(w1_h.at[:, pl.ds(o, FU)], wb.at[slot, :, pl.ds(0, FU)], us.at[slot, 0]),
                pltpu.make_async_copy(w3_h.at[:, pl.ds(o, FU)], wb.at[slot, :, pl.ds(FU, FU)], us.at[slot, 1])]

    def down(t, slot):
        return pltpu.make_async_copy(w2_h.at[:, pl.ds(pl.multiple_of(t * ND, 128), ND)], w2b.at[slot], ds.at[slot])

    hl = [pltpu.make_async_copy(hpb_h, hall.at[2], ld.at[0]),
          pltpu.make_async_copy(h_h.at[pl.ds(0, PC)], hall.at[0], ld.at[1]),
          pltpu.make_async_copy(h_h.at[pl.ds(PC, PC)], hall.at[1], ld.at[2])]
    hl[0].start()
    for cp in up(0, 0):
        cp.start()
    for cp in hl[1:]:
        cp.start()

    bar = pltpu.get_barrier_semaphore()
    pl.semaphore_signal(bar, inc=1, device_id=YP, device_id_type=MESH)
    pl.semaphore_wait(bar, 1)
    hsend = rc(h_h.at[pl.ds(PC, PC)], hall.at[3], zsem.at[2], zrm.at[2])
    hsend.start()
    zc = [rc(zs.at[i], zr.at[i], zsem.at[i], zrm.at[i]) for i in range(2)]
    oc = [pltpu.make_async_copy(hall.at[i], o_h.at[pl.ds(i * PC, PC)], ld.at[3 + i]) for i in range(2)]

    def finish(i):
        zc[i].wait_recv()

        def blk(t, _):
            r = pl.ds(pl.multiple_of(t * 128, 128), 128)
            y = hall[i, r, :].astype(jnp.float32) + (zo[i, r, :] + zr[i, r, :].astype(jnp.float32))
            hall[i, r, :] = y.astype(jnp.bfloat16)
            return 0

        lax.fori_loop(0, PC // 128, blk, 0)
        oc[i].start()

    def chunk(ci, _):
        peer = ci % 2 == 0
        half = ci // 2
        idx = jnp.where(peer, 2, 0) + half

        @pl.when(ci == 0)
        def _():
            hl[0].wait()

        @pl.when(ci == 1)
        def _():
            hl[1].wait()

        @pl.when(ci == 2)
        def _():
            hsend.wait_recv()

        @pl.when(ci == 3)
        def _():
            hl[2].wait()

        b_s[...] = rms(hall[idx], g_ref[...])

        @pl.when(ci == 1)
        def _():
            zc[0].start()

        @pl.when(ci == 3)
        def _():
            zc[1].start()
            finish(0)

        def ustep(t, _):
            n = ci * NU_ + t
            slot = n % 2
            last = t == NU_ - 1

            @pl.when(jnp.logical_not(jnp.logical_and(last, ci == 3)))
            def _():
                for cp in up(jnp.where(last, 0, t + 1), 1 - slot):
                    cp.start()

            @pl.when(t == NU_ - 2)
            def _():
                down(0, (ci * NDN) % 2).start()

            for cp in up(t, slot):
                cp.wait()
            y = jnp.dot(b_s[...], wb[slot], preferred_element_type=jnp.float32)
            a = y[:, :FU]
            hid[:, pl.ds(pl.multiple_of(t * FU, 128), FU)] = (a * jax.nn.sigmoid(a) * y[:, FU:]).astype(jnp.bfloat16)
            return 0

        lax.fori_loop(0, NU_, ustep, 0)

        def dstep(t, _):
            n = ci * NDN + t
            slot = n % 2

            @pl.when(t < NDN - 1)
            def _():
                down(t + 1, 1 - slot).start()

            down(t, slot).wait()
            y = jnp.dot(hid[...], w2b[slot], preferred_element_type=jnp.float32)
            cols = pl.ds(pl.multiple_of(t * ND, 128), ND)

            @pl.when(peer)
            def _():
                zs[half, :, cols] = y.astype(jnp.bfloat16)

            @pl.when(jnp.logical_not(peer))
            def _():
                zo[half, :, cols] = y

            return 0

        lax.fori_loop(0, NDN, dstep, 0)
        return 0

    lax.fori_loop(0, 4, chunk, 0)
    finish(1)
    hsend.wait_send()
    for i in range(2):
        zc[i].wait_send()
        oc[i].wait()


def mlp(h, hpb, g, w1, w3, w2):
    n = h.shape[0]
    f = w1.shape[1]
    any_ = pl.BlockSpec(memory_space=pl.ANY)
    bf, f32 = jnp.bfloat16, jnp.float32
    return pl.pallas_call(
        mlp_kernel,
        in_specs=[any_, any_, pl.BlockSpec(memory_space=pltpu.VMEM), any_, any_, any_],
        out_specs=any_,
        out_shape=jax.ShapeDtypeStruct((n, D), bf),
        scratch_shapes=[
            pltpu.VMEM((4, PC, D), bf), pltpu.VMEM((2, D, 2 * FU), bf), pltpu.VMEM((2, f, ND), bf),
            pltpu.VMEM((PC, f), bf), pltpu.VMEM((PC, D), bf), pltpu.VMEM((2, PC, D), bf), pltpu.VMEM((2, PC, D), bf),
            pltpu.VMEM((2, PC, D), f32),
            pltpu.SemaphoreType.DMA((5,)), pltpu.SemaphoreType.DMA((2, 2)), pltpu.SemaphoreType.DMA((2,)),
            pltpu.SemaphoreType.DMA((3,)), pltpu.SemaphoreType.DMA((3,))],
        compiler_params=pltpu.CompilerParams(collective_id=1, has_side_effects=True, vmem_limit_bytes=VM),
        cost_estimate=cost(12 * n * D * f, 24 * D * f), name="mlp")(h, hpb, g, w1, w3, w2)


def solution(mesh):
    tok = P(('dp', 'cp', 'tp'), None)
    col = P(None, 'tp')
    row = P('tp', None)

    def local(x, pos, g1, g2, wq, wk, wv, wo, w1, w3, w2):
        freq = 1.0 / (THETA ** (jnp.arange(0, DH, 2, dtype=jnp.float32) / DH))
        ang = pos.astype(jnp.float32)[:, None] * freq
        cs = jnp.cos(ang)
        sn = jnp.sin(ang)
        cs = jnp.concatenate([cs, cs], 1)
        sn = jnp.concatenate([-sn, sn], 1)
        h, hp = att(x, g1.reshape(1, D), cs, sn, wq, wk, wv, wo)
        return mlp(h, hp, g2.reshape(1, D), w1, w3, w2)

    return jax.shard_map(local, mesh=mesh, in_specs=(tok, P(('dp', 'cp', 'tp')), P(None), P(None), col, col, col, row, col, col, row), out_specs=tok, check_vma=False)
```

```python
import functools
import math
import jax
import jax.numpy as jnp
from jax import lax
from jax.experimental import pallas as pl
from jax.experimental.pallas import tpu as pltpu
from jax.sharding import PartitionSpec as P

DH = 128
EPS = 1e-5
THETA = 500000.0
NEG = -1e30
LC = math.log2(math.e) / math.sqrt(DH)
PC = 512
GRP = 6
D = 1536
QW = GRP * DH
VM = 62 * 2**20
MESH = pl.DeviceIdType.MESH


def cost(flops, byts, tr=0):
    return pl.CostEstimate(flops=int(flops), bytes_accessed=int(byts), transcendentals=int(tr))


def rms(v, g):
    vf = v.astype(jnp.float32)
    inv = lax.rsqrt(jnp.mean(vf * vf, axis=-1, keepdims=True) + EPS)
    return (vf * inv * g.astype(jnp.float32)).astype(jnp.bfloat16)


def att_kernel(x_h, g_ref, cs_h, sn_h, wq_h, wk_h, wv_h, wo_h,
               h_ref, hp_ref,
               xv, csv, snv, wqb, wkb, wvb, wob, qb, kvb, m_s, al_s, acc_s, s0, s1, p0, p1, ob, hs,
               ld, ks, kr, ws, wr, hsem):
    c = lax.axis_index('cp')
    j = lax.axis_index('tp')
    core = lax.rem(c, 2)
    k = c * 2 + j
    cs_ = c + 1 - 2 * core
    cx = lax.rem(c + 2, 4)
    cxs = lax.rem(cs_ + 2, 4)
    SIB = {"cp": cs_}
    XP = {"cp": cx}
    YP = {"tp": 1 - j}
    S = [s0, s1]
    PP = [p0, p1]

    def rc(src, dst, ss, rs, dev):
        return pltpu.make_async_remote_copy(src_ref=src, dst_ref=dst, send_sem=ss, recv_sem=rs, device_id=dev, device_id_type=MESH)

    loads = [(x_h, xv), (wq_h, wqb.at[0]), (wk_h, wkb.at[0]), (wv_h, wvb.at[0]), (cs_h, csv), (sn_h, snv)]
    loads = [pltpu.make_async_copy(a, b, ld.at[i]) for i, (a, b) in enumerate(loads)]
    wol = pltpu.make_async_copy(wo_h, wob.at[pl.ds(0, QW)], ld.at[6])
    for l in loads:
        l.start()

    bar = pltpu.get_barrier_semaphore()
    for d in (SIB, XP, YP):
        pl.semaphore_signal(bar, inc=1, device_id=d, device_id_type=MESH)
    pl.semaphore_wait(bar, 3)

    W = {'k': (wk_h, wkb.at[1], 2, 0, 1), 'v': (wv_h, wvb.at[1], 2, 0, 1), 'qa': (wq_h, wqb.at[1], 4, 0, 2),
         'qb': (wq_h, wqb.at[1], 4, 1, 2), 'o': (wo_h, wob.at[pl.ds(QW, QW)], 2, 0, 1)}
    WI = {n: i for i, n in enumerate(W)}

    def wrange(n, q):
        src, dst, div, sub, nsub = W[n]
        r = src.shape[0] // div
        return pl.ds(pl.multiple_of(q * r + sub * (r // nsub), r // nsub), r // nsub)

    def wcopy(n, hop):
        src, dst, div, sub, nsub = W[n]
        q = core if div == 2 else (c if hop < 3 else cx)
        rg = wrange(n, q)
        i = WI[n]
        return rc((src if hop == 0 else dst).at[rg], dst.at[rg], ws.at[i, hop], wr.at[i, hop], (YP, SIB, XP, SIB)[hop])

    def wrecv(n, hop):
        src, dst, div, sub, nsub = W[n]
        q = (core, 1 - core)[hop] if div == 2 else (c, cs_, cx, cxs)[hop]
        rg = wrange(n, q)
        i = WI[n]
        rc(dst.at[rg], dst.at[rg], ws.at[i, hop], wr.at[i, hop], (YP, SIB, XP, SIB)[hop]).wait_recv()

    KV = {'S': (0, 0, 0, 2, SIB), 'X': (0, 0, 0, 4, XP), 'Y': (0, 0, 1, 1, YP), 'XS': (0, 4, 0, 6, SIB),
          'YS': (1, 1, 1, 3, SIB), 'Z': (1, 1, 1, 5, XP), 'ZS': (1, 5, 1, 7, SIB),
          's': (1, 0, 1, 2, SIB), 'x': (1, 0, 1, 4, XP), 'y': (1, 0, 0, 1, YP), 'xs': (1, 4, 1, 6, SIB),
          'ys': (0, 1, 0, 3, SIB), 'z': (0, 1, 0, 5, XP), 'zs': (0, 5, 0, 7, SIB)}

    def kcopy(n):
        gs, ms, gd, md, dev = KV[n]
        return rc(kvb.at[gs, ms], kvb.at[gd, md], ks.at[gd, md], kr.at[gd, md], dev)

    for n in ('k', 'v', 'qa'):
        wcopy(n, 0).start()
    for l in loads:
        l.wait()
    wol.start()

    def front(g, do_q, do_kv):
        def blk(i, _):
            r = pl.ds(pl.multiple_of(i * 256, 256), 256)
            a = rms(xv[r, :], g_ref[0:1, :])
            ww = ([wqb[g]] if do_q else []) + ([wkb[g], wvb[g]] if do_kv else [])
            y = jnp.dot(a, jnp.concatenate(ww, axis=1) if len(ww) > 1 else ww[0], preferred_element_type=jnp.float32)
            cc = csv[r, :]
            sc = snv[r, :]

            def rot(h):
                u = y[:, h * DH:(h + 1) * DH]
                return (u * cc + pltpu.roll(u, DH // 2, 1) * sc).astype(jnp.bfloat16)

            if do_q:
                for h in range(GRP):
                    qb[g, r, h * DH:(h + 1) * DH] = rot(h)
            if do_kv:
                n = GRP if do_q else 0
                kvb[g, 0, r, :DH] = rot(n)
                kvb[g, 0, r, DH:] = y[:, (n + 1) * DH:(n + 2) * DH].astype(jnp.bfloat16)
            return 0

        lax.fori_loop(0, 4, blk, 0)

    front(0, True, True)
    for n in 'SX':
        kcopy(n).start()

    m_s[...] = jnp.full_like(m_s, NEG)
    acc_s[...] = jnp.zeros_like(acc_s)
    al_s[...] = jnp.ones_like(al_s)
    p1[...] = jnp.zeros_like(p1)
    ones = jnp.ones((PC, 128), jnp.bfloat16)

    two = lambda g, ms: [(g, m, t) for m in ms for t in (3, 4)]
    late = (2, 1, 3, 4, 6, 5, 7)
    seq = [(0, 0, 0), (0, 0, 1), (0, 0, 2)] + two(0, (2, 4, 6, 1, 3, 5, 7)) + [(1, 0, 0)] + [(1, m, 3) for m in late]
    seq = seq + [(1, 0, 1), (1, 0, 2)] + [(1, m, 4) for m in late]
    NU = len(seq)
    codes = [g * 64 + m * 8 + t for g, m, t in seq]

    def code_of(u):
        v = jnp.int32(codes[0])
        for i in range(1, NU):
            v = jnp.where(u == i, codes[i], v)
        return v

    def decode(cd):
        g = cd // 64
        m = (cd // 8) % 8
        t = cd % 8
        lt = jnp.where(m >= 4, k // 4, jnp.where(m >= 2, (k // 2) % 2, k % 2))
        qp = jnp.where(t == 0, 0, jnp.where(t == 3, 1 - lt, 1))
        hf = jnp.where(t == 1, 1, jnp.where(t == 4, 1 - lt, 0))
        return g, m, t, qp, hf

    def qk(e, h):
        g, m, t, qp, hf = e
        qo = pl.multiple_of(qp * PC, PC)
        ko = pl.multiple_of(hf * PC, PC)
        S[h % 2][...] = lax.dot_general(qb[g, pl.ds(qo, PC), h * DH:(h + 1) * DH], kvb[g, m, pl.ds(ko, PC), :DH],
                                        (((1,), (1,)), ((), ())), preferred_element_type=jnp.float32)

    def sm(e, h, masked):
        g, m, t, qp, hf = e
        s = S[h % 2][...]
        if masked:
            r = lax.broadcasted_iota(jnp.int32, s.shape, 0)
            cc = lax.broadcasted_iota(jnp.int32, s.shape, 1)
            s = jnp.where(cc <= r, s, NEG)
        mx = jnp.max(s, axis=1, keepdims=True)
        mp = m_s[g, qp, h]
        mn = jnp.maximum(mp, mx)
        al_s[h % 2] = jnp.exp2((mp - mn) * LC)
        pr = jnp.exp2(s * LC - jnp.tile(mn * LC, (1, PC // 128)))
        PP[h % 2][...] = pr.astype(jnp.bfloat16)
        m_s[g, qp, h] = mn

    def pv(e, h):
        g, m, t, qp, hf = e
        ko = pl.multiple_of(hf * PC, PC)
        vb = jnp.concatenate([kvb[g, m, pl.ds(ko, PC), DH:], ones], axis=1)
        y = jnp.dot(PP[h % 2][...], vb, preferred_element_type=jnp.float32)
        acc_s[g, qp, h] = acc_s[g, qp, h] * jnp.tile(al_s[h % 2], (1, 2)) + y

    def finalize(qp):
        for g in range(2):
            for h in range(GRP):
                a = acc_s[g, qp, h]
                ob[:, (g * GRP + h) * DH:(g * GRP + h + 1) * DH] = (a[:, :128] / a[:, 128:]).astype(jnp.bfloat16)

        def blk(i, _):
            r = pl.ds(pl.multiple_of(i * 256, 256), 256)
            rx = pl.ds(pl.multiple_of(qp * PC + i * 256, 256), 256)
            y = jnp.dot(ob[r, :], wob[...], preferred_element_type=jnp.float32)
            hs[rx, :] = (xv[rx, :].astype(jnp.float32) + y).astype(jnp.bfloat16)
            return 0

        lax.fori_loop(0, 2, blk, 0)

    hcopy = rc(hs.at[pl.ds(0, PC)], hp_ref, hsem.at[0], hsem.at[1], YP)
    hout = [pltpu.make_async_copy(hs.at[pl.ds(i * PC, PC)], h_ref.at[pl.ds(i * PC, PC)], ld.at[7 + i]) for i in range(2)]

    kw = lambda n: kcopy(n).wait_recv()

    def act(u):
        def at(i):
            return pl.when(u == i)

        @at(2)
        def _():
            for n in 'kv':
                wrecv(n, 0)
                wcopy(n, 1).start()
            kw('S')

        @at(3)
        def _():
            for n in 'kv':
                wrecv(n, 1)
            front(1, False, True)
            kcopy('s').start()
            kcopy('y').start()
            wcopy('qb', 0).start()
            kcopy('Y').start()

        @at(4)
        def _():
            kw('X')
            kcopy('XS').start()
            wrecv('qa', 0)
            wcopy('qa', 2).start()
            wcopy('qa', 1).start()

        @at(6)
        def _():
            kw('XS')

        @at(8)
        def _():
            kw('y')
            kcopy('ys').start()
            kcopy('z').start()

        @at(10)
        def _():
            kw('ys')

        @at(11)
        def _():
            wrecv('qb', 0)
            wcopy('qb', 2).start()
            wcopy('qb', 1).start()
            kcopy('x').start()
            wcopy('o', 0).start()

        @at(12)
        def _():
            kw('z')
            kcopy('zs').start()

        @at(14)
        def _():
            kw('zs')
            wrecv('qa', 2)
            wcopy('qa', 3).start()

        @at(15)
        def _():
            kw('Y')
            kcopy('YS').start()
            kcopy('Z').start()

        @at(16)
        def _():
            wrecv('qb', 2)
            wcopy('qb', 3).start()
            kw('s')
            for n in ('qa', 'qb'):
                wrecv(n, 1)
                wrecv(n, 3)
            front(1, True, False)

        @at(19)
        def _():
            kw('YS')

        @at(20)
        def _():
            kw('x')
            kcopy('xs').start()

        @at(21)
        def _():
            kw('xs')

        @at(22)
        def _():
            kw('Z')
            kcopy('ZS').start()

        @at(23)
        def _():
            kw('ZS')

        @at(24)
        def _():
            wrecv('o', 0)
            wcopy('o', 1).start()

        @at(26)
        def _():
            wol.wait()
            wrecv('o', 1)
            finalize(0)
            hcopy.start()
            hout[0].start()

    e0 = decode(jnp.int32(codes[0]))
    qk(e0, 0)

    def body(u, carry):
        cc, pc = carry
        act(u)
        nc = code_of(jnp.minimum(u + 1, NU - 1))
        cur, prv, nxt = decode(cc), decode(pc), decode(nc)

        def run(masked):
            for h in range(GRP):
                if h < GRP - 1:
                    qk(cur, h + 1)
                else:
                    qk(nxt, 0)
                if h == 0:
                    pv(prv, GRP - 1)
                else:
                    pv(cur, h - 1)
                sm(cur, h, masked)

        diag = cur[2] < 2

        @pl.when(diag)
        def _():
            run(True)

        @pl.when(jnp.logical_not(diag))
        def _():
            run(False)

        return nc, cc

    fin = lax.fori_loop(0, NU, body, (jnp.int32(codes[0]), jnp.int32(codes[0])))
    pv(decode(fin[1]), GRP - 1)
    finalize(1)
    hout[1].start()
    hcopy.wait_recv()
    hcopy.wait_send()
    for o in hout:
        o.wait()
    for n in KV:
        kcopy(n).wait_send()
    for n in W:
        for hop in range(W[n][2]):
            wcopy(n, hop).wait_send()


def att(x, g, cs, sn, wq, wk, wv, wo):
    n = x.shape[0]
    any_ = pl.BlockSpec(memory_space=pl.ANY)
    vm = pl.BlockSpec(memory_space=pltpu.VMEM)
    bf, f32 = jnp.bfloat16, jnp.float32
    return pl.pallas_call(
        att_kernel,
        in_specs=[any_, vm] + [any_] * 6,
        out_specs=[any_, any_],
        out_shape=[jax.ShapeDtypeStruct((n, D), bf), jax.ShapeDtypeStruct((PC, D), bf)],
        scratch_shapes=[
            pltpu.VMEM((n, D), bf), pltpu.VMEM((n, DH), f32), pltpu.VMEM((n, DH), f32),
            pltpu.VMEM((2, D, QW), bf), pltpu.VMEM((2, D, DH), bf), pltpu.VMEM((2, D, DH), bf), pltpu.VMEM((D, D), bf),
            pltpu.VMEM((2, n, QW), bf), pltpu.VMEM((2, 8, n, 2 * DH), bf),
            pltpu.VMEM((2, 2, GRP, PC, 128), f32), pltpu.VMEM((2, PC, 128), f32), pltpu.VMEM((2, 2, GRP, PC, 256), f32),
            pltpu.VMEM((PC, PC), f32), pltpu.VMEM((PC, PC), f32), pltpu.VMEM((PC, PC), bf), pltpu.VMEM((PC, PC), bf),
            pltpu.VMEM((PC, D), bf), pltpu.VMEM((n, D), bf),
            pltpu.SemaphoreType.DMA((9,)), pltpu.SemaphoreType.DMA((2, 8)), pltpu.SemaphoreType.DMA((2, 8)),
            pltpu.SemaphoreType.DMA((5, 4)), pltpu.SemaphoreType.DMA((5, 4)), pltpu.SemaphoreType.DMA((2,))],
        compiler_params=pltpu.CompilerParams(collective_id=0, has_side_effects=True, vmem_limit_bytes=VM),
        cost_estimate=cost(70e9, 20 * 2**20), name="att")(x, g, cs, sn, wq, wk, wv, wo)


FU = 896
ND = 768


def mlp_kernel(h_h, hpb_h, g_ref, w1_h, w3_h, w2_h, o_h, hall, wb, w2b, hid, b_s, zs, zr, zo, ld, us, ds, zsem, zrm):
    j = lax.axis_index('tp')
    YP = {"tp": 1 - j}
    F = w1_h.shape[1]
    NU_, NDN = F // FU, D // ND

    def rc(src, dst, ss, rs):
        return pltpu.make_async_remote_copy(src_ref=src, dst_ref=dst, send_sem=ss, recv_sem=rs, device_id=YP, device_id_type=MESH)

    def up(t, slot):
        o = pl.multiple_of(t * FU, 128)
        return [pltpu.make_async_copy(w1_h.at[:, pl.ds(o, FU)], wb.at[slot, :, pl.ds(0, FU)], us.at[slot, 0]),
                pltpu.make_async_copy(w3_h.at[:, pl.ds(o, FU)], wb.at[slot, :, pl.ds(FU, FU)], us.at[slot, 1])]

    def down(t, slot):
        return pltpu.make_async_copy(w2_h.at[:, pl.ds(pl.multiple_of(t * ND, 128), ND)], w2b.at[slot], ds.at[slot])

    hl = [pltpu.make_async_copy(hpb_h, hall.at[2], ld.at[0]),
          pltpu.make_async_copy(h_h.at[pl.ds(0, PC)], hall.at[0], ld.at[1]),
          pltpu.make_async_copy(h_h.at[pl.ds(PC, PC)], hall.at[1], ld.at[2])]
    hl[0].start()
    for cp in up(0, 0):
        cp.start()
    for cp in hl[1:]:
        cp.start()

    bar = pltpu.get_barrier_semaphore()
    pl.semaphore_signal(bar, inc=1, device_id=YP, device_id_type=MESH)
    pl.semaphore_wait(bar, 1)
    hsend = rc(h_h.at[pl.ds(PC, PC)], hall.at[3], zsem.at[2], zrm.at[2])
    hsend.start()
    zc = [rc(zs.at[i], zr.at[i], zsem.at[i], zrm.at[i]) for i in range(2)]
    oc = [pltpu.make_async_copy(hall.at[i], o_h.at[pl.ds(i * PC, PC)], ld.at[3 + i]) for i in range(2)]

    def finish(i):
        zc[i].wait_recv()

        def blk(t, _):
            r = pl.ds(pl.multiple_of(t * 128, 128), 128)
            y = hall[i, r, :].astype(jnp.float32) + (zo[i, r, :] + zr[i, r, :].astype(jnp.float32))
            hall[i, r, :] = y.astype(jnp.bfloat16)
            return 0

        lax.fori_loop(0, PC // 128, blk, 0)
        oc[i].start()

    def up_phase(n, idx, hb, more, pre):
        b_s[...] = rms(hall[idx], g_ref[1:2, :])

        def step(t, _):
            slot = (n * NU_ + t) % 2
            last = t == NU_ - 1

            @pl.when(jnp.logical_or(more, jnp.logical_not(last)))
            def _():
                for cp in up(jnp.where(last, 0, t + 1), 1 - slot):
                    cp.start()

            if pre is not None:
                @pl.when(t == NU_ - 2)
                def _():
                    down(0, pre).start()

            for cp in up(t, slot):
                cp.wait()
            y = jnp.dot(b_s[...], wb[slot], preferred_element_type=jnp.float32)
            a = y[:, :FU]
            hid[hb, :, pl.ds(pl.multiple_of(t * FU, 128), FU)] = (a * jax.nn.sigmoid(a) * y[:, FU:]).astype(jnp.bfloat16)
            return 0

        lax.fori_loop(0, NU_, step, 0)

    def down_phase(n, idx, hb, chain):
        def step(t, _):
            slot = (n * NDN + t) % 2

            @pl.when(jnp.logical_or(chain, t < NDN - 1))
            def _():
                down(jnp.where(t == NDN - 1, 0, t + 1), 1 - slot).start()

            down(t, slot).wait()
            y = jnp.dot(hid[hb], w2b[slot], preferred_element_type=jnp.float32)
            cols = pl.ds(pl.multiple_of(t * ND, 128), ND)
            if idx >= 2:
                zs[idx - 2, :, cols] = y.astype(jnp.bfloat16)
            else:
                zo[idx, :, cols] = y
            return 0

        lax.fori_loop(0, NDN, step, 0)

    hl[0].wait()
    up_phase(0, 2, 0, True, 0)
    down_phase(0, 2, 0, False)
    hl[1].wait()
    zc[0].start()
    up_phase(1, 0, 1, True, None)
    hsend.wait_recv()
    up_phase(2, 3, 0, True, NDN % 2)
    down_phase(1, 3, 0, True)
    hl[2].wait()
    zc[1].start()
    down_phase(2, 0, 1, False)
    finish(0)
    up_phase(3, 1, 0, False, (3 * NDN) % 2)
    down_phase(3, 1, 0, False)
    finish(1)
    hsend.wait_send()
    for i in range(2):
        zc[i].wait_send()
        oc[i].wait()


def mlp(h, hpb, g, w1, w3, w2):
    n = h.shape[0]
    f = w1.shape[1]
    any_ = pl.BlockSpec(memory_space=pl.ANY)
    bf, f32 = jnp.bfloat16, jnp.float32
    return pl.pallas_call(
        mlp_kernel,
        in_specs=[any_, any_, pl.BlockSpec(memory_space=pltpu.VMEM), any_, any_, any_],
        out_specs=any_,
        out_shape=jax.ShapeDtypeStruct((n, D), bf),
        scratch_shapes=[
            pltpu.VMEM((4, PC, D), bf), pltpu.VMEM((2, D, 2 * FU), bf), pltpu.VMEM((2, f, ND), bf),
            pltpu.VMEM((2, PC, f), bf), pltpu.VMEM((PC, D), bf), pltpu.VMEM((2, PC, D), bf), pltpu.VMEM((2, PC, D), bf),
            pltpu.VMEM((2, PC, D), f32),
            pltpu.SemaphoreType.DMA((5,)), pltpu.SemaphoreType.DMA((2, 2)), pltpu.SemaphoreType.DMA((2,)),
            pltpu.SemaphoreType.DMA((3,)), pltpu.SemaphoreType.DMA((3,))],
        compiler_params=pltpu.CompilerParams(collective_id=1, has_side_effects=True, vmem_limit_bytes=VM),
        cost_estimate=cost(12 * n * D * f, 24 * D * f), name="mlp")(h, hpb, g, w1, w3, w2)


def solution(mesh):
    tok = P(('dp', 'cp', 'tp'), None)
    col = P(None, 'tp')
    row = P('tp', None)

    def local(x, pos, g1, g2, wq, wk, wv, wo, w1, w3, w2):
        freq = 1.0 / (THETA ** (jnp.arange(0, DH, 2, dtype=jnp.float32) / DH))
        ang = pos.astype(jnp.float32)[:, None] * freq
        cs = jnp.cos(ang)
        sn = jnp.sin(ang)
        cs = jnp.concatenate([cs, cs], 1)
        sn = jnp.concatenate([-sn, sn], 1)
        gs = jnp.stack([g1, g2])
        h, hp = att(x, gs, cs, sn, wq, wk, wv, wo)
        return mlp(h, hp, gs, w1, w3, w2)

    return jax.shard_map(local, mesh=mesh, in_specs=(tok, P(('dp', 'cp', 'tp')), P(None), P(None), col, col, col, row, col, col, row), out_specs=tok, check_vma=False)
```

```python
import functools
import math
import jax
import jax.numpy as jnp
import numpy as np
from jax import lax
from jax.experimental import pallas as pl
from jax.experimental.pallas import tpu as pltpu
from jax.sharding import PartitionSpec as P

DH = 128
EPS = 1e-5
THETA = 500000.0
NEG = -1e30
LC = math.log2(math.e) / math.sqrt(DH)
PC = 512
GRP = 6
D = 1536
QW = GRP * DH
VM = 62 * 2**20
MESH = pl.DeviceIdType.MESH


def cost(flops, byts, tr=0):
    return pl.CostEstimate(flops=int(flops), bytes_accessed=int(byts), transcendentals=int(tr))


def rms(v, g):
    vf = v.astype(jnp.float32)
    inv = lax.rsqrt(jnp.mean(vf * vf, axis=-1, keepdims=True) + EPS)
    return (vf * inv * g.astype(jnp.float32)).astype(jnp.bfloat16)


def att_kernel(x_h, g_ref, pos_ref, fr_ref, wq_h, wk_h, wv_h, wo_h,
               h_ref, hp_ref,
               xv, csv, snv, wqb, wkb, wvb, wob, qb, kvb, m_s, al_s, acc_s, s0, s1, p0, p1, ob, hs,
               ld, ks, kr, ws, wr, hsem):
    c = lax.axis_index('cp')
    j = lax.axis_index('tp')
    core = lax.rem(c, 2)
    k = c * 2 + j
    cs_ = c + 1 - 2 * core
    cx = lax.rem(c + 2, 4)
    cxs = lax.rem(cs_ + 2, 4)
    SIB = {"cp": cs_}
    XP = {"cp": cx}
    YP = {"tp": 1 - j}
    S = [s0, s1]
    PP = [p0, p1]

    def rc(src, dst, ss, rs, dev):
        return pltpu.make_async_remote_copy(src_ref=src, dst_ref=dst, send_sem=ss, recv_sem=rs, device_id=dev, device_id_type=MESH)

    loads = [(x_h, xv), (wq_h, wqb.at[0]), (wk_h, wkb.at[0]), (wv_h, wvb.at[0])]
    loads = [pltpu.make_async_copy(a, b, ld.at[i]) for i, (a, b) in enumerate(loads)]
    wol = pltpu.make_async_copy(wo_h, wob.at[pl.ds(0, QW)], ld.at[6])
    for l in loads:
        l.start()

    bar = pltpu.get_barrier_semaphore()
    for d in (SIB, XP, YP):
        pl.semaphore_signal(bar, inc=1, device_id=d, device_id_type=MESH)
    pl.semaphore_wait(bar, 3)

    W = {'k': (wk_h, wkb.at[1], 2, 0, 1), 'v': (wv_h, wvb.at[1], 2, 0, 1), 'qa': (wq_h, wqb.at[1], 4, 0, 2),
         'qb': (wq_h, wqb.at[1], 4, 1, 2), 'o': (wo_h, wob.at[pl.ds(QW, QW)], 2, 0, 1)}
    WI = {n: i for i, n in enumerate(W)}

    def wrange(n, q):
        src, dst, div, sub, nsub = W[n]
        r = src.shape[0] // div
        return pl.ds(pl.multiple_of(q * r + sub * (r // nsub), r // nsub), r // nsub)

    def wcopy(n, hop):
        src, dst, div, sub, nsub = W[n]
        q = core if div == 2 else (c if hop < 3 else cx)
        rg = wrange(n, q)
        i = WI[n]
        return rc((src if hop == 0 else dst).at[rg], dst.at[rg], ws.at[i, hop], wr.at[i, hop], (YP, SIB, XP, SIB)[hop])

    def wrecv(n, hop):
        src, dst, div, sub, nsub = W[n]
        q = (core, 1 - core)[hop] if div == 2 else (c, cs_, cx, cxs)[hop]
        rg = wrange(n, q)
        i = WI[n]
        rc(dst.at[rg], dst.at[rg], ws.at[i, hop], wr.at[i, hop], (YP, SIB, XP, SIB)[hop]).wait_recv()

    KV = {'S': (0, 0, 0, 2, SIB), 'X': (0, 0, 0, 4, XP), 'Y': (0, 0, 1, 1, YP), 'XS': (0, 4, 0, 6, SIB),
          'YS': (1, 1, 1, 3, SIB), 'Z': (1, 1, 1, 5, XP), 'ZS': (1, 5, 1, 7, SIB),
          's': (1, 0, 1, 2, SIB), 'x': (1, 0, 1, 4, XP), 'y': (1, 0, 0, 1, YP), 'xs': (1, 4, 1, 6, SIB),
          'ys': (0, 1, 0, 3, SIB), 'z': (0, 1, 0, 5, XP), 'zs': (0, 5, 0, 7, SIB)}

    def kcopy(n):
        gs, ms, gd, md, dev = KV[n]
        return rc(kvb.at[gs, ms], kvb.at[gd, md], ks.at[gd, md], kr.at[gd, md], dev)

    for n in ('k', 'v', 'qa', 'qb'):
        wcopy(n, 0).start()

    sign = jnp.where(lax.broadcasted_iota(jnp.int32, (128, DH), 1) < DH // 2, -1.0, 1.0)

    def table(i, _):
        r = pl.ds(pl.multiple_of(i * 128, 128), 128)
        p = jnp.broadcast_to(pos_ref[pl.ds(i, 1), :].astype(jnp.float32), (128, 128)).T
        ang = p * fr_ref[...]
        csv[r, :] = jnp.cos(ang)
        snv[r, :] = jnp.sin(ang) * sign
        return 0

    lax.fori_loop(0, x_h.shape[0] // 128, table, 0)
    for l in loads:
        l.wait()
    wol.start()

    def front(g, do_q, do_kv):
        def blk(i, _):
            r = pl.ds(pl.multiple_of(i * 256, 256), 256)
            a = rms(xv[r, :], g_ref[...].reshape(1, D))
            ww = ([wqb[g]] if do_q else []) + ([wkb[g], wvb[g]] if do_kv else [])
            y = jnp.dot(a, jnp.concatenate(ww, axis=1) if len(ww) > 1 else ww[0], preferred_element_type=jnp.float32)
            cc = csv[r, :]
            sc = snv[r, :]

            def rot(h):
                u = y[:, h * DH:(h + 1) * DH]
                return (u * cc + pltpu.roll(u, DH // 2, 1) * sc).astype(jnp.bfloat16)

            if do_q:
                for h in range(GRP):
                    qb[g, r, h * DH:(h + 1) * DH] = rot(h)
            if do_kv:
                n = GRP if do_q else 0
                kvb[g, 0, r, :DH] = rot(n)
                kvb[g, 0, r, DH:] = y[:, (n + 1) * DH:(n + 2) * DH].astype(jnp.bfloat16)
            return 0

        lax.fori_loop(0, 4, blk, 0)

    front(0, True, True)
    for n in 'SX':
        kcopy(n).start()

    m_s[...] = jnp.full_like(m_s, NEG)
    acc_s[...] = jnp.zeros_like(acc_s)
    al_s[...] = jnp.ones_like(al_s)
    p1[...] = jnp.zeros_like(p1)
    ones = jnp.ones((PC, 128), jnp.bfloat16)

    two = lambda g, ms: [(g, m, t) for m in ms for t in (3, 4)]
    own = lambda g: [(g, 0, 0), (g, 0, 1), (g, 0, 2)]
    seq = own(0) + two(0, (2, 4, 6)) + own(1) + [(1, 2, 3), (0, 1, 3), (0, 3, 3), (1, 1, 3), (1, 3, 3), (0, 5, 3), (0, 7, 3)]
    seq = seq + [(1, m, 3) for m in (4, 6, 5, 7)]
    NB = len(seq)
    seq = seq + [(1, m, 4) for m in (2, 1, 3, 4, 6, 5, 7)] + [(0, m, 4) for m in (1, 3, 5, 7)]
    NU = len(seq)
    codes = [g * 64 + m * 8 + t for g, m, t in seq]

    def code_of(u):
        v = jnp.int32(codes[0])
        for i in range(1, NU):
            v = jnp.where(u == i, codes[i], v)
        return v

    def decode(cd):
        g = cd // 64
        m = (cd // 8) % 8
        t = cd % 8
        lt = jnp.where(m >= 4, k // 4, jnp.where(m >= 2, (k // 2) % 2, k % 2))
        qp = jnp.where(t == 0, 0, jnp.where(t == 3, 1 - lt, 1))
        hf = jnp.where(t == 1, 1, jnp.where(t == 4, 1 - lt, 0))
        return g, m, t, qp, hf

    def qk(e, h):
        g, m, t, qp, hf = e
        qo = pl.multiple_of(qp * PC, PC)
        ko = pl.multiple_of(hf * PC, PC)
        S[h % 2][...] = lax.dot_general(qb[g, pl.ds(qo, PC), h * DH:(h + 1) * DH], kvb[g, m, pl.ds(ko, PC), :DH],
                                        (((1,), (1,)), ((), ())), preferred_element_type=jnp.float32)

    def sm(e, h, masked):
        g, m, t, qp, hf = e
        s = S[h % 2][...]
        if masked:
            r = lax.broadcasted_iota(jnp.int32, s.shape, 0)
            cc = lax.broadcasted_iota(jnp.int32, s.shape, 1)
            s = jnp.where(cc <= r, s, NEG)
        mx = jnp.max(s, axis=1, keepdims=True)
        mp = m_s[g, qp, h]
        mn = jnp.maximum(mp, mx)
        al_s[h % 2] = jnp.exp2((mp - mn) * LC)
        pr = jnp.exp2(s * LC - jnp.tile(mn * LC, (1, PC // 128)))
        PP[h % 2][...] = pr.astype(jnp.bfloat16)
        m_s[g, qp, h] = mn

    def pv(e, h):
        g, m, t, qp, hf = e
        ko = pl.multiple_of(hf * PC, PC)
        vb = jnp.concatenate([kvb[g, m, pl.ds(ko, PC), DH:], ones], axis=1)
        y = jnp.dot(PP[h % 2][...], vb, preferred_element_type=jnp.float32)
        acc_s[g, qp, h] = acc_s[g, qp, h] * jnp.tile(al_s[h % 2], (1, 2)) + y

    def finalize(qp):
        for g in range(2):
            for h in range(GRP):
                a = acc_s[g, qp, h]
                ob[:, (g * GRP + h) * DH:(g * GRP + h + 1) * DH] = (a[:, :128] / a[:, 128:]).astype(jnp.bfloat16)

        def blk(i, _):
            r = pl.ds(pl.multiple_of(i * 256, 256), 256)
            rx = pl.ds(pl.multiple_of(qp * PC + i * 256, 256), 256)
            y = jnp.dot(ob[r, :], wob[...], preferred_element_type=jnp.float32)
            hs[rx, :] = (xv[rx, :].astype(jnp.float32) + y).astype(jnp.bfloat16)
            return 0

        lax.fori_loop(0, 2, blk, 0)

    hcopy = rc(hs.at[pl.ds(0, PC)], hp_ref, hsem.at[0], hsem.at[1], YP)
    hout = [pltpu.make_async_copy(hs.at[pl.ds(i * PC, PC)], h_ref.at[pl.ds(i * PC, PC)], ld.at[7 + i]) for i in range(2)]

    kw = lambda n: kcopy(n).wait_recv()

    def act(u, prv):
        def at(i):
            return pl.when(u == i)

        @at(2)
        def _():
            for n in 'kv':
                wrecv(n, 0)
                wcopy(n, 1).start()
            kw('S')

        @at(3)
        def _():
            for n in 'kv':
                wrecv(n, 1)
            front(1, False, True)
            kcopy('s').start()
            kcopy('y').start()
            kcopy('Y').start()

        @at(4)
        def _():
            kw('X')
            kcopy('XS').start()
            wrecv('qa', 0)
            wcopy('qa', 2).start()
            wcopy('qa', 1).start()

        @at(6)
        def _():
            kw('XS')
            wrecv('qb', 0)
            wcopy('qb', 2).start()
            wcopy('qb', 1).start()

        @at(8)
        def _():
            wrecv('qa', 2)
            wcopy('qa', 3).start()
            wrecv('qb', 2)
            wcopy('qb', 3).start()
            kw('y')
            kcopy('ys').start()
            kcopy('z').start()
            for n in ('qa', 'qb'):
                wrecv(n, 1)
                wrecv(n, 3)
            front(1, True, False)

        @at(9)
        def _():
            kcopy('x').start()
            wcopy('o', 0).start()

        @at(11)
        def _():
            kw('s')

        @at(12)
        def _():
            kw('Y')
            kcopy('YS').start()
            kcopy('Z').start()

        @at(13)
        def _():
            kw('ys')

        @at(14)
        def _():
            kw('z')
            kcopy('zs').start()

        @at(15)
        def _():
            kw('YS')

        @at(17)
        def _():
            kw('zs')
            kw('x')
            kcopy('xs').start()

        @at(19)
        def _():
            kw('xs')

        @at(20)
        def _():
            kw('Z')
            kcopy('ZS').start()

        @at(21)
        def _():
            wrecv('o', 0)
            wcopy('o', 1).start()
            kw('ZS')

        @at(NB)
        def _():
            pv(prv, GRP - 1)
            p1[...] = jnp.zeros_like(p1)
            al_s[1] = jnp.ones_like(al_s[1])
            wol.wait()
            wrecv('o', 1)
            finalize(0)
            hcopy.start()
            hout[0].start()

    e0 = decode(jnp.int32(codes[0]))
    qk(e0, 0)

    def body(u, carry):
        cc, pc = carry
        nc = code_of(jnp.minimum(u + 1, NU - 1))
        cur, prv, nxt = decode(cc), decode(pc), decode(nc)
        act(u, prv)

        def run(masked):
            for h in range(GRP):
                if h < GRP - 1:
                    qk(cur, h + 1)
                else:
                    qk(nxt, 0)
                if h == 0:
                    pv(prv, GRP - 1)
                else:
                    pv(cur, h - 1)
                sm(cur, h, masked)

        diag = cur[2] < 2

        @pl.when(diag)
        def _():
            run(True)

        @pl.when(jnp.logical_not(diag))
        def _():
            run(False)

        return nc, cc

    fin = lax.fori_loop(0, NU, body, (jnp.int32(codes[0]), jnp.int32(codes[0])))
    pv(decode(fin[1]), GRP - 1)
    finalize(1)
    hout[1].start()
    hcopy.wait_recv()
    hcopy.wait_send()
    for o in hout:
        o.wait()
    for n in KV:
        kcopy(n).wait_send()
    for n in W:
        for hop in range(W[n][2]):
            wcopy(n, hop).wait_send()


def att(x, g, pos, fr, wq, wk, wv, wo):
    n = x.shape[0]
    any_ = pl.BlockSpec(memory_space=pl.ANY)
    vm = pl.BlockSpec(memory_space=pltpu.VMEM)
    bf, f32 = jnp.bfloat16, jnp.float32
    return pl.pallas_call(
        att_kernel,
        in_specs=[any_, vm, vm, vm] + [any_] * 4,
        out_specs=[any_, any_],
        out_shape=[jax.ShapeDtypeStruct((n, D), bf), jax.ShapeDtypeStruct((PC, D), bf)],
        scratch_shapes=[
            pltpu.VMEM((n, D), bf), pltpu.VMEM((n, DH), f32), pltpu.VMEM((n, DH), f32),
            pltpu.VMEM((2, D, QW), bf), pltpu.VMEM((2, D, DH), bf), pltpu.VMEM((2, D, DH), bf), pltpu.VMEM((D, D), bf),
            pltpu.VMEM((2, n, QW), bf), pltpu.VMEM((2, 8, n, 2 * DH), bf),
            pltpu.VMEM((2, 2, GRP, PC, 128), f32), pltpu.VMEM((2, PC, 128), f32), pltpu.VMEM((2, 2, GRP, PC, 256), f32),
            pltpu.VMEM((PC, PC), f32), pltpu.VMEM((PC, PC), f32), pltpu.VMEM((PC, PC), bf), pltpu.VMEM((PC, PC), bf),
            pltpu.VMEM((PC, D), bf), pltpu.VMEM((n, D), bf),
            pltpu.SemaphoreType.DMA((9,)), pltpu.SemaphoreType.DMA((2, 8)), pltpu.SemaphoreType.DMA((2, 8)),
            pltpu.SemaphoreType.DMA((5, 4)), pltpu.SemaphoreType.DMA((5, 4)), pltpu.SemaphoreType.DMA((2,))],
        compiler_params=pltpu.CompilerParams(collective_id=0, has_side_effects=True, vmem_limit_bytes=VM),
        cost_estimate=cost(70e9, 20 * 2**20), name="att")(x, g, pos, fr, wq, wk, wv, wo)


FU = 896
ND = 768


def mlp_kernel(h_h, hpb_h, g_ref, w1_h, w3_h, w2_h, ob_h, oa_h, hall, wb, w2b, hid, b_s, zs, zr, zo, ld, us, ds, os_, zsem, zrm):
    j = lax.axis_index('tp')
    YP = {"tp": 1 - j}
    F = w1_h.shape[1]
    NU_, NDN = F // FU, D // ND

    def rc(src, dst, ss, rs):
        return pltpu.make_async_remote_copy(src_ref=src, dst_ref=dst, send_sem=ss, recv_sem=rs, device_id=YP, device_id_type=MESH)

    def up(t, slot):
        o = pl.multiple_of(t * FU, 128)
        return [pltpu.make_async_copy(w1_h.at[:, pl.ds(o, FU)], wb.at[slot, :, pl.ds(0, FU)], us.at[slot, 0]),
                pltpu.make_async_copy(w3_h.at[:, pl.ds(o, FU)], wb.at[slot, :, pl.ds(FU, FU)], us.at[slot, 1])]

    def down(t, slot):
        return pltpu.make_async_copy(w2_h.at[:, pl.ds(pl.multiple_of(t * ND, 128), ND)], w2b.at[slot], ds.at[slot])

    hl = [pltpu.make_async_copy(hpb_h, hall.at[2], ld.at[0]),
          pltpu.make_async_copy(h_h.at[pl.ds(0, PC)], hall.at[0], ld.at[1]),
          pltpu.make_async_copy(h_h.at[pl.ds(PC, PC)], hall.at[1], ld.at[2])]
    hl[0].start()
    for cp in up(0, 0):
        cp.start()
    for cp in hl[1:]:
        cp.start()

    bar = pltpu.get_barrier_semaphore()
    pl.semaphore_signal(bar, inc=1, device_id=YP, device_id_type=MESH)
    pl.semaphore_wait(bar, 1)
    hsend = rc(h_h.at[pl.ds(PC, PC)], hall.at[3], zsem.at[2], zrm.at[2])
    hsend.start()
    hp = PC // 2
    zc = [rc(zs.at[0], zr.at[0], zsem.at[0], zrm.at[0])]
    zc = zc + [rc(zs.at[1, pl.ds(i * hp, hp)], zr.at[1, pl.ds(i * hp, hp)], zsem.at[(1, 3)[i]], zrm.at[(1, 3)[i]]) for i in range(2)]
    outs = (ob_h, oa_h)
    oc = [pltpu.make_async_copy(hall.at[i, pl.ds(r, hp)], outs[i].at[pl.ds(r, hp)], os_.at[i, r // hp]) for i in range(2) for r in (0, hp)]

    def finish(i, part):
        def blk(t, _):
            r = pl.ds(pl.multiple_of(part * hp + t * 128, 128), 128)
            y = hall[i, r, :].astype(jnp.float32) + (zo[i, r, :] + zr[i, r, :].astype(jnp.float32))
            hall[i, r, :] = y.astype(jnp.bfloat16)
            return 0

        lax.fori_loop(0, hp // 128, blk, 0)
        oc[2 * i + part].start()

    def up_phase(n, idx, hb, more, pre):
        b_s[...] = rms(hall[idx], g_ref[...].reshape(1, D))

        def step(t, _):
            slot = (n * NU_ + t) % 2
            last = t == NU_ - 1

            @pl.when(jnp.logical_or(more, jnp.logical_not(last)))
            def _():
                for cp in up(jnp.where(last, 0, t + 1), 1 - slot):
                    cp.start()

            if pre is not None:
                @pl.when(t == NU_ - 2)
                def _():
                    down(0, pre).start()

            for cp in up(t, slot):
                cp.wait()
            y = jnp.dot(b_s[...], wb[slot], preferred_element_type=jnp.float32)
            a = y[:, :FU]
            hid[hb, :, pl.ds(pl.multiple_of(t * FU, 128), FU)] = (a * jax.nn.sigmoid(a) * y[:, FU:]).astype(jnp.bfloat16)
            return 0

        lax.fori_loop(0, NU_, step, 0)

    def down_phase(n, idx, hb, chain):
        def step(t, _):
            slot = (n * NDN + t) % 2

            @pl.when(jnp.logical_or(chain, t < NDN - 1))
            def _():
                down(jnp.where(t == NDN - 1, 0, t + 1), 1 - slot).start()

            down(t, slot).wait()
            y = jnp.dot(hid[hb], w2b[slot], preferred_element_type=jnp.float32)
            cols = pl.ds(pl.multiple_of(t * ND, 128), ND)
            if idx >= 2:
                zs[idx - 2, :, cols] = y.astype(jnp.bfloat16)
            else:
                zo[idx, :, cols] = y
            return 0

        lax.fori_loop(0, NDN, step, 0)

    hl[0].wait()
    up_phase(0, 2, 0, True, 0)
    down_phase(0, 2, 0, False)
    hl[1].wait()
    zc[0].start()
    up_phase(1, 0, 1, True, None)
    hsend.wait_recv()
    up_phase(2, 3, 0, True, NDN % 2)
    down_phase(1, 3, 0, True)
    zc[1].start()
    zc[2].start()
    down_phase(2, 0, 1, False)
    zc[0].wait_recv()
    finish(0, 0)
    finish(0, 1)
    hl[2].wait()
    up_phase(3, 1, 0, False, (3 * NDN) % 2)
    down_phase(3, 1, 0, False)
    for i in range(2):
        zc[1 + i].wait_recv()
        finish(1, i)
    for o in oc:
        o.wait()
    hsend.wait_send()
    for z in zc:
        z.wait_send()


def mlp(h, hpb, g, w1, w3, w2):
    n = h.shape[0]
    f = w1.shape[1]
    any_ = pl.BlockSpec(memory_space=pl.ANY)
    bf, f32 = jnp.bfloat16, jnp.float32
    return pl.pallas_call(
        mlp_kernel,
        in_specs=[any_, any_, pl.BlockSpec(memory_space=pltpu.VMEM), any_, any_, any_],
        out_specs=[any_] * 2,
        out_shape=[jax.ShapeDtypeStruct((PC, D), bf)] * 2,
        scratch_shapes=[
            pltpu.VMEM((4, PC, D), bf), pltpu.VMEM((2, D, 2 * FU), bf), pltpu.VMEM((2, f, ND), bf),
            pltpu.VMEM((2, PC, f), bf), pltpu.VMEM((PC, D), bf), pltpu.VMEM((2, PC, D), bf), pltpu.VMEM((2, PC, D), bf),
            pltpu.VMEM((2, PC, D), f32),
            pltpu.SemaphoreType.DMA((3,)), pltpu.SemaphoreType.DMA((2, 2)), pltpu.SemaphoreType.DMA((2,)), pltpu.SemaphoreType.DMA((2, 2)),
            pltpu.SemaphoreType.DMA((4,)), pltpu.SemaphoreType.DMA((4,))],
        compiler_params=pltpu.CompilerParams(collective_id=1, has_side_effects=True, vmem_limit_bytes=VM),
        cost_estimate=cost(12 * n * D * f, 24 * D * f), name="mlp")(h, hpb, g, w1, w3, w2)


def solution(mesh):
    tok = P(('dp', 'cp', 'tp'), None)
    col = P(None, 'tp')
    row = P('tp', None)

    def local(x, pos, g1, g2, wq, wk, wv, wo, w1, w3, w2):
        fr = 1.0 / (np.float32(THETA) ** (np.arange(0, DH, 2, dtype=np.float32) / np.float32(DH)))
        fr = jnp.asarray(np.concatenate([fr, fr]).astype(np.float32).reshape(1, DH))
        h, hp = att(x, g1, pos.reshape(-1, 128), fr, wq, wk, wv, wo)
        return jnp.concatenate(mlp(h, hp, g2, w1, w3, w2), 0)

    return jax.shard_map(local, mesh=mesh, in_specs=(tok, P(('dp', 'cp', 'tp')), P(None), P(None), col, col, col, row, col, col, row), out_specs=tok, check_vma=False)
```

```python
import functools
import math
import re
import jax
import jax.numpy as jnp
import numpy as np
from jax import lax
from jax.experimental import pallas as pl
from jax.experimental.pallas import tpu as pltpu
from jax.sharding import PartitionSpec as P

DH = 128
EPS = 1e-5
THETA = 500000.0
NEG = -1e30
LC = math.log2(math.e) / math.sqrt(DH)
PC = 512
GRP = 6
D = 1536
QW = GRP * DH
VM = 62 * 2**20
MESH = pl.DeviceIdType.MESH


def cost(flops, byts, tr=0):
    return pl.CostEstimate(flops=int(flops), bytes_accessed=int(byts), transcendentals=int(tr))


def rms(v, g):
    vf = v.astype(jnp.float32)
    inv = lax.rsqrt(jnp.mean(vf * vf, axis=-1, keepdims=True) + EPS)
    return (vf * inv * g.astype(jnp.float32)).astype(jnp.bfloat16)


def att_kernel(x_h, g_ref, pos_ref, fr_ref, wq_h, wk_h, wv_h, wo_h,
               h_ref, hp_ref,
               xv, csv, snv, wqb, wkb, wvb, wob, qb, kvb, m_s, al_s, acc_s, s0, s1, p0, p1, ob, hs,
               ld, ks, kr, ws, wr, hsem):
    c = lax.axis_index('cp')
    j = lax.axis_index('tp')
    core = lax.rem(c, 2)
    k = c * 2 + j
    cs_ = c + 1 - 2 * core
    cx = lax.rem(c + 2, 4)
    cxs = lax.rem(cs_ + 2, 4)
    SIB = {"cp": cs_}
    XP = {"cp": cx}
    YP = {"tp": 1 - j}
    S = [s0, s1]
    PP = [p0, p1]

    def rc(src, dst, ss, rs, dev):
        return pltpu.make_async_remote_copy(src_ref=src, dst_ref=dst, send_sem=ss, recv_sem=rs, device_id=dev, device_id_type=MESH)

    loads = [(x_h, xv), (wq_h, wqb.at[0]), (wk_h, wkb.at[0]), (wv_h, wvb.at[0])]
    loads = [pltpu.make_async_copy(a, b, ld.at[i]) for i, (a, b) in enumerate(loads)]
    wol = pltpu.make_async_copy(wo_h, wob.at[pl.ds(0, QW)], ld.at[6])
    for l in loads:
        l.start()

    bar = pltpu.get_barrier_semaphore()
    for d in (SIB, XP, YP):
        pl.semaphore_signal(bar, inc=1, device_id=d, device_id_type=MESH)
    pl.semaphore_wait(bar, 3)

    W = {'k': (wk_h, wkb.at[1], 2, 0, 1), 'v': (wv_h, wvb.at[1], 2, 0, 1), 'qa': (wq_h, wqb.at[1], 4, 0, 2),
         'qb': (wq_h, wqb.at[1], 4, 1, 2), 'o': (wo_h, wob.at[pl.ds(QW, QW)], 2, 0, 1)}
    WI = {n: i for i, n in enumerate(W)}

    def wrange(n, q):
        src, dst, div, sub, nsub = W[n]
        r = src.shape[0] // div
        return pl.ds(pl.multiple_of(q * r + sub * (r // nsub), r // nsub), r // nsub)

    def wcopy(n, hop):
        src, dst, div, sub, nsub = W[n]
        q = core if div == 2 else (c if hop < 3 else cx)
        rg = wrange(n, q)
        i = WI[n]
        return rc((src if hop == 0 else dst).at[rg], dst.at[rg], ws.at[i, hop], wr.at[i, hop], (YP, SIB, XP, SIB)[hop])

    def wrecv(n, hop):
        src, dst, div, sub, nsub = W[n]
        q = (core, 1 - core)[hop] if div == 2 else (c, cs_, cx, cxs)[hop]
        rg = wrange(n, q)
        i = WI[n]
        rc(dst.at[rg], dst.at[rg], ws.at[i, hop], wr.at[i, hop], (YP, SIB, XP, SIB)[hop]).wait_recv()

    KV = {'S': '0002S', 'X': '0004X', 'Y': '0011Y', 'XS': '0406S', 'YS': '1113S', 'Z': '1115X', 'ZS': '1517S',
          's': '1012S', 'x': '1014X', 'y': '1001Y', 'xs': '1416S', 'ys': '0103S', 'z': '0105X', 'zs': '0507S'}
    PEER = {'S': SIB, 'X': XP, 'Y': YP}

    def kcopy(n):
        (gs, ms, gd, md), dev = map(int, KV[n][:-1]), PEER[KV[n][-1]]
        return rc(kvb.at[gs, ms], kvb.at[gd, md], ks.at[gd, md], kr.at[gd, md], dev)

    for n in ('k', 'v', 'qa', 'qb'):
        wcopy(n, 0).start()

    sign = jnp.where(lax.broadcasted_iota(jnp.int32, (128, DH), 1) < DH // 2, -1.0, 1.0)

    def table(i, _):
        r = pl.ds(pl.multiple_of(i * 128, 128), 128)
        p = jnp.broadcast_to(pos_ref[pl.ds(i, 1), :].astype(jnp.float32), (128, 128)).T
        ang = p * fr_ref[...]
        csv[r, :] = jnp.cos(ang)
        snv[r, :] = jnp.sin(ang) * sign
        return 0

    lax.fori_loop(0, x_h.shape[0] // 128, table, 0)
    for l in loads:
        l.wait()
    wol.start()

    def front(g, do_q, do_kv):
        def blk(i, _):
            r = pl.ds(pl.multiple_of(i * 256, 256), 256)
            a = rms(xv[r, :], g_ref[...].reshape(1, D))
            ww = ([wqb[g]] if do_q else []) + ([wkb[g], wvb[g]] if do_kv else [])
            y = jnp.dot(a, jnp.concatenate(ww, axis=1) if len(ww) > 1 else ww[0], preferred_element_type=jnp.float32)
            cc = csv[r, :]
            sc = snv[r, :]

            def rot(h):
                u = y[:, h * DH:(h + 1) * DH]
                return (u * cc + pltpu.roll(u, DH // 2, 1) * sc).astype(jnp.bfloat16)

            if do_q:
                for h in range(GRP):
                    qb[g, r, h * DH:(h + 1) * DH] = rot(h)
            if do_kv:
                n = GRP if do_q else 0
                kvb[g, 0, r, :DH] = rot(n)
                kvb[g, 0, r, DH:] = y[:, (n + 1) * DH:(n + 2) * DH].astype(jnp.bfloat16)
            return 0

        lax.fori_loop(0, 4, blk, 0)

    front(0, True, True)
    for n in 'SX':
        kcopy(n).start()

    m_s[...] = jnp.full_like(m_s, NEG)
    acc_s[...] = jnp.zeros_like(acc_s)
    al_s[...] = jnp.ones_like(al_s)
    p1[...] = jnp.zeros_like(p1)
    ones = jnp.ones((PC, 128), jnp.bfloat16)

    EARLY = '000001002023024043044063064100123013033113133053073143163101' + '102153173'
    LATE = '124114134144164154174014034054074'
    NB = len(EARLY) // 3
    codes = [int(c[0]) * 64 + int(c[1]) * 8 + int(c[2]) for c in re.findall('...', EARLY + LATE)]
    NU = len(codes)

    def code_of(u):
        v = jnp.int32(codes[0])
        for i in range(1, NU):
            v = jnp.where(u == i, codes[i], v)
        return v

    def decode(cd):
        g = cd // 64
        m = (cd // 8) % 8
        t = cd % 8
        lt = jnp.where(m >= 4, k // 4, jnp.where(m >= 2, (k // 2) % 2, k % 2))
        qp = jnp.where(t == 0, 0, jnp.where(t == 3, 1 - lt, 1))
        hf = jnp.where(t == 1, 1, jnp.where(t == 4, 1 - lt, 0))
        return g, m, t, qp, hf

    def qk(e, h):
        g, m, t, qp, hf = e
        qo = pl.multiple_of(qp * PC, PC)
        ko = pl.multiple_of(hf * PC, PC)
        S[h % 2][...] = lax.dot_general(qb[g, pl.ds(qo, PC), h * DH:(h + 1) * DH], kvb[g, m, pl.ds(ko, PC), :DH],
                                        (((1,), (1,)), ((), ())), preferred_element_type=jnp.float32)

    def sm(e, h, masked):
        g, m, t, qp, hf = e
        s = S[h % 2][...]
        if masked:
            r = lax.broadcasted_iota(jnp.int32, s.shape, 0)
            cc = lax.broadcasted_iota(jnp.int32, s.shape, 1)
            s = jnp.where(cc <= r, s, NEG)
        mx = jnp.max(s, axis=1, keepdims=True)
        mp = m_s[g, qp, h]
        mn = jnp.maximum(mp, mx)
        al_s[h % 2] = jnp.exp2((mp - mn) * LC)
        pr = jnp.exp2(s * LC - jnp.tile(mn * LC, (1, PC // 128)))
        PP[h % 2][...] = pr.astype(jnp.bfloat16)
        m_s[g, qp, h] = mn

    def pv(e, h):
        g, m, t, qp, hf = e
        ko = pl.multiple_of(hf * PC, PC)
        vb = jnp.concatenate([kvb[g, m, pl.ds(ko, PC), DH:], ones], axis=1)
        y = jnp.dot(PP[h % 2][...], vb, preferred_element_type=jnp.float32)
        acc_s[g, qp, h] = acc_s[g, qp, h] * jnp.tile(al_s[h % 2], (1, 2)) + y

    def finalize(qp):
        for g in range(2):
            for h in range(GRP):
                a = acc_s[g, qp, h]
                ob[:, (g * GRP + h) * DH:(g * GRP + h + 1) * DH] = (a[:, :128] / a[:, 128:]).astype(jnp.bfloat16)

        def blk(i, _):
            r = pl.ds(pl.multiple_of(i * 256, 256), 256)
            rx = pl.ds(pl.multiple_of(qp * PC + i * 256, 256), 256)
            y = jnp.dot(ob[r, :], wob[...], preferred_element_type=jnp.float32)
            hs[rx, :] = (xv[rx, :].astype(jnp.float32) + y).astype(jnp.bfloat16)
            if qp == 0:
                hcopy(i).start()
            return 0

        lax.fori_loop(0, 2, blk, 0)

    def hcopy(i):
        r = pl.ds(pl.multiple_of(i * 256, 256), 256)
        return rc(hs.at[r], hp_ref.at[r], hsem.at[0, i], hsem.at[1, i], YP)

    hout = [pltpu.make_async_copy(hs.at[pl.ds(i * PC, PC)], h_ref.at[pl.ds(i * PC, PC)], ld.at[7 + i]) for i in range(2)]

    kw = lambda n: kcopy(n).wait_recv()

    def act(u, prv):
        def at(i):
            return pl.when(u == i)

        @at(2)
        def _():
            for n in 'kv':
                wrecv(n, 0)
                wcopy(n, 1).start()
            kw('S')

        @at(3)
        def _():
            for n in 'kv':
                wrecv(n, 1)
            front(1, False, True)
            kcopy('s').start()
            kcopy('y').start()
            kcopy('Y').start()

        @at(4)
        def _():
            kw('X')
            kcopy('XS').start()
            wrecv('qa', 0)
            wcopy('qa', 2).start()
            wcopy('qa', 1).start()

        @at(6)
        def _():
            kw('XS')
            wrecv('qb', 0)
            wcopy('qb', 2).start()
            wcopy('qb', 1).start()

        @at(8)
        def _():
            wrecv('qa', 2)
            wcopy('qa', 3).start()
            wrecv('qb', 2)
            wcopy('qb', 3).start()
            kw('y')
            kcopy('ys').start()
            kcopy('z').start()
            for n in ('qa', 'qb'):
                wrecv(n, 1)
                wrecv(n, 3)
            front(1, True, False)

        @at(9)
        def _():
            kcopy('x').start()
            wcopy('o', 0).start()
            kw('s')

        @at(10)
        def _():
            kw('Y')
            kcopy('YS').start()
            kcopy('Z').start()

        @at(11)
        def _():
            kw('ys')

        @at(12)
        def _():
            kw('z')
            kcopy('zs').start()

        @at(13)
        def _():
            kw('YS')

        @at(15)
        def _():
            kw('zs')

        @at(16)
        def _():
            kw('x')
            kcopy('xs').start()

        @at(17)
        def _():
            kw('xs')

        @at(20)
        def _():
            kw('Z')
            kcopy('ZS').start()

        @at(21)
        def _():
            wrecv('o', 0)
            wcopy('o', 1).start()
            kw('ZS')

        @at(NB)
        def _():
            pv(prv, GRP - 1)
            p1[...] = jnp.zeros_like(p1)
            al_s[1] = jnp.ones_like(al_s[1])
            wol.wait()
            wrecv('o', 1)
            finalize(0)
            hout[0].start()

    e0 = decode(jnp.int32(codes[0]))
    qk(e0, 0)

    def body(u, carry):
        cc, pc = carry
        nc = code_of(jnp.minimum(u + 1, NU - 1))
        cur, prv, nxt = decode(cc), decode(pc), decode(nc)
        act(u, prv)

        def run(masked):
            for h in range(GRP):
                if h < GRP - 1:
                    qk(cur, h + 1)
                else:
                    qk(nxt, 0)
                if h == 0:
                    pv(prv, GRP - 1)
                else:
                    pv(cur, h - 1)
                sm(cur, h, masked)

        diag = cur[2] < 2

        @pl.when(diag)
        def _():
            run(True)

        @pl.when(jnp.logical_not(diag))
        def _():
            run(False)

        return nc, cc

    fin = lax.fori_loop(0, NU, body, (jnp.int32(codes[0]), jnp.int32(codes[0])))
    pv(decode(fin[1]), GRP - 1)
    finalize(1)
    hout[1].start()
    for i in range(2):
        hcopy(i).wait_recv()
        hcopy(i).wait_send()
    for o in hout:
        o.wait()
    for n in KV:
        kcopy(n).wait_send()
    for n in W:
        for hop in range(W[n][2]):
            wcopy(n, hop).wait_send()


def att(x, g, pos, fr, wq, wk, wv, wo):
    n = x.shape[0]
    any_ = pl.BlockSpec(memory_space=pl.ANY)
    vm = pl.BlockSpec(memory_space=pltpu.VMEM)
    bf, f32 = jnp.bfloat16, jnp.float32
    return pl.pallas_call(
        att_kernel,
        in_specs=[any_, vm, vm, vm] + [any_] * 4,
        out_specs=[any_, any_],
        out_shape=[jax.ShapeDtypeStruct((n, D), bf), jax.ShapeDtypeStruct((PC, D), bf)],
        scratch_shapes=[
            pltpu.VMEM((n, D), bf), pltpu.VMEM((n, DH), f32), pltpu.VMEM((n, DH), f32),
            pltpu.VMEM((2, D, QW), bf), pltpu.VMEM((2, D, DH), bf), pltpu.VMEM((2, D, DH), bf), pltpu.VMEM((D, D), bf),
            pltpu.VMEM((2, n, QW), bf), pltpu.VMEM((2, 8, n, 2 * DH), bf),
            pltpu.VMEM((2, 2, GRP, PC, 128), f32), pltpu.VMEM((2, PC, 128), f32), pltpu.VMEM((2, 2, GRP, PC, 256), f32),
            pltpu.VMEM((PC, PC), f32), pltpu.VMEM((PC, PC), f32), pltpu.VMEM((PC, PC), bf), pltpu.VMEM((PC, PC), bf),
            pltpu.VMEM((PC, D), bf), pltpu.VMEM((n, D), bf),
            pltpu.SemaphoreType.DMA((9,)), pltpu.SemaphoreType.DMA((2, 8)), pltpu.SemaphoreType.DMA((2, 8)),
            pltpu.SemaphoreType.DMA((5, 4)), pltpu.SemaphoreType.DMA((5, 4)), pltpu.SemaphoreType.DMA((2, 2))],
        compiler_params=pltpu.CompilerParams(collective_id=0, has_side_effects=True, vmem_limit_bytes=VM),
        cost_estimate=cost(70e9, 20 * 2**20), name="att")(x, g, pos, fr, wq, wk, wv, wo)


FU = 896
ND = 768


def mlp_kernel(h_h, hpb_h, g_ref, w1_h, w3_h, w2_h, ob_h, oa_h, hall, wb, w2b, hid, b_s, zs, zr, zo, ld, us, ds, os_, zsem, zrm):
    j = lax.axis_index('tp')
    YP = {"tp": 1 - j}
    F = w1_h.shape[1]
    NU_, NDN = F // FU, D // ND

    def rc(src, dst, ss, rs):
        return pltpu.make_async_remote_copy(src_ref=src, dst_ref=dst, send_sem=ss, recv_sem=rs, device_id=YP, device_id_type=MESH)

    def up(t, slot):
        o = pl.multiple_of(t * FU, 128)
        return [pltpu.make_async_copy(w1_h.at[:, pl.ds(o, FU)], wb.at[slot, :, pl.ds(0, FU)], us.at[slot, 0]),
                pltpu.make_async_copy(w3_h.at[:, pl.ds(o, FU)], wb.at[slot, :, pl.ds(FU, FU)], us.at[slot, 1])]

    def down(t, slot):
        return pltpu.make_async_copy(w2_h.at[:, pl.ds(pl.multiple_of(t * ND, 128), ND)], w2b.at[slot], ds.at[slot])

    hl = [pltpu.make_async_copy(hpb_h, hall.at[2], ld.at[0]),
          pltpu.make_async_copy(h_h.at[pl.ds(0, PC)], hall.at[0], ld.at[1]),
          pltpu.make_async_copy(h_h.at[pl.ds(PC, PC)], hall.at[1], ld.at[2])]
    hl[0].start()
    for cp in up(0, 0):
        cp.start()
    for cp in hl[1:]:
        cp.start()

    bar = pltpu.get_barrier_semaphore()
    pl.semaphore_signal(bar, inc=1, device_id=YP, device_id_type=MESH)
    pl.semaphore_wait(bar, 1)
    hsend = rc(h_h.at[pl.ds(PC, PC)], hall.at[3], zsem.at[2], zrm.at[2])
    hsend.start()
    hp = PC // 2
    zc = [rc(zs.at[0], zr.at[0], zsem.at[0], zrm.at[0])]
    zc = zc + [rc(zs.at[1, pl.ds(i * hp, hp)], zr.at[1, pl.ds(i * hp, hp)], zsem.at[(1, 3)[i]], zrm.at[(1, 3)[i]]) for i in range(2)]
    outs = (ob_h, oa_h)
    oc = [pltpu.make_async_copy(hall.at[i, pl.ds(r, hp)], outs[i].at[pl.ds(r, hp)], os_.at[i, r // hp]) for i in range(2) for r in (0, hp)]

    def finish(i, part):
        def blk(t, _):
            r = pl.ds(pl.multiple_of(part * hp + t * 128, 128), 128)
            y = hall[i, r, :].astype(jnp.float32) + (zo[i, r, :] + zr[i, r, :].astype(jnp.float32))
            hall[i, r, :] = y.astype(jnp.bfloat16)
            return 0

        lax.fori_loop(0, hp // 128, blk, 0)
        oc[2 * i + part].start()

    def up_phase(n, idx, hb, more, pre):
        b_s[...] = rms(hall[idx], g_ref[...].reshape(1, D))

        def step(t, _):
            slot = (n * NU_ + t) % 2
            last = t == NU_ - 1

            @pl.when(jnp.logical_or(more, jnp.logical_not(last)))
            def _():
                for cp in up(jnp.where(last, 0, t + 1), 1 - slot):
                    cp.start()

            if pre is not None:
                @pl.when(t == NU_ - 2)
                def _():
                    down(0, pre).start()

            for cp in up(t, slot):
                cp.wait()
            y = jnp.dot(b_s[...], wb[slot], preferred_element_type=jnp.float32)
            a = y[:, :FU]
            hid[hb, :, pl.ds(pl.multiple_of(t * FU, 128), FU)] = (a * jax.nn.sigmoid(a) * y[:, FU:]).astype(jnp.bfloat16)
            return 0

        lax.fori_loop(0, NU_, step, 0)

    def down_phase(n, idx, hb, chain):
        def step(t, _):
            slot = (n * NDN + t) % 2

            @pl.when(jnp.logical_or(chain, t < NDN - 1))
            def _():
                down(jnp.where(t == NDN - 1, 0, t + 1), 1 - slot).start()

            down(t, slot).wait()
            y = jnp.dot(hid[hb], w2b[slot], preferred_element_type=jnp.float32)
            cols = pl.ds(pl.multiple_of(t * ND, 128), ND)
            if idx >= 2:
                zs[idx - 2, :, cols] = y.astype(jnp.bfloat16)
            else:
                zo[idx, :, cols] = y
            return 0

        lax.fori_loop(0, NDN, step, 0)

    hl[0].wait()
    up_phase(0, 2, 0, True, 0)
    down_phase(0, 2, 0, False)
    hl[1].wait()
    zc[0].start()
    up_phase(1, 0, 1, True, None)
    hsend.wait_recv()
    up_phase(2, 3, 0, True, NDN % 2)
    down_phase(1, 3, 0, True)
    zc[1].start()
    zc[2].start()
    down_phase(2, 0, 1, False)
    zc[0].wait_recv()
    finish(0, 0)
    finish(0, 1)
    hl[2].wait()
    up_phase(3, 1, 0, False, (3 * NDN) % 2)
    down_phase(3, 1, 0, False)
    for i in range(2):
        zc[1 + i].wait_recv()
        finish(1, i)
    for o in oc:
        o.wait()
    hsend.wait_send()
    for z in zc:
        z.wait_send()


def mlp(h, hpb, g, w1, w3, w2):
    n = h.shape[0]
    f = w1.shape[1]
    any_ = pl.BlockSpec(memory_space=pl.ANY)
    bf, f32 = jnp.bfloat16, jnp.float32
    return pl.pallas_call(
        mlp_kernel,
        in_specs=[any_, any_, pl.BlockSpec(memory_space=pltpu.VMEM), any_, any_, any_],
        out_specs=[any_] * 2,
        out_shape=[jax.ShapeDtypeStruct((PC, D), bf)] * 2,
        scratch_shapes=[
            pltpu.VMEM((4, PC, D), bf), pltpu.VMEM((2, D, 2 * FU), bf), pltpu.VMEM((2, f, ND), bf),
            pltpu.VMEM((2, PC, f), bf), pltpu.VMEM((PC, D), bf), pltpu.VMEM((2, PC, D), bf), pltpu.VMEM((2, PC, D), bf),
            pltpu.VMEM((2, PC, D), f32),
            pltpu.SemaphoreType.DMA((3,)), pltpu.SemaphoreType.DMA((2, 2)), pltpu.SemaphoreType.DMA((2,)), pltpu.SemaphoreType.DMA((2, 2)),
            pltpu.SemaphoreType.DMA((4,)), pltpu.SemaphoreType.DMA((4,))],
        compiler_params=pltpu.CompilerParams(collective_id=1, has_side_effects=True, vmem_limit_bytes=VM),
        cost_estimate=cost(12 * n * D * f, 24 * D * f), name="mlp")(h, hpb, g, w1, w3, w2)


def solution(mesh):
    tok = P(('dp', 'cp', 'tp'), None)
    col = P(None, 'tp')
    row = P('tp', None)

    def local(x, pos, g1, g2, wq, wk, wv, wo, w1, w3, w2):
        fr = 1.0 / (np.float32(THETA) ** (np.arange(0, DH, 2, dtype=np.float32) / np.float32(DH)))
        fr = jnp.asarray(np.concatenate([fr, fr]).astype(np.float32).reshape(1, DH))
        h, hp = att(x, g1, pos.reshape(-1, 128), fr, wq, wk, wv, wo)
        return jnp.concatenate(mlp(h, hp, g2, w1, w3, w2), 0)

    return jax.shard_map(local, mesh=mesh, in_specs=(tok, P(('dp', 'cp', 'tp')), P(None), P(None), col, col, col, row, col, col, row), out_specs=tok, check_vma=False)
```

```python
import functools
import math
import re
import jax
import jax.numpy as jnp
import numpy as np
from jax import lax
from jax.experimental import pallas as pl
from jax.experimental.pallas import tpu as pltpu
from jax.sharding import PartitionSpec as P

DH = 128
EPS = 1e-5
THETA = 500000.0
NEG = -1e30
LC = math.log2(math.e) / math.sqrt(DH)
PC = 512
GRP = 6
D = 1536
QW = GRP * DH
VM = 62 * 2**20
MESH = pl.DeviceIdType.MESH


def cost(flops, byts, tr=0):
    return pl.CostEstimate(flops=int(flops), bytes_accessed=int(byts), transcendentals=int(tr))


def rms(v, g):
    vf = v.astype(jnp.float32)
    inv = lax.rsqrt(jnp.mean(vf * vf, axis=-1, keepdims=True) + EPS)
    return (vf * inv * g.astype(jnp.float32)).astype(jnp.bfloat16)


def att_kernel(x_h, g_ref, pos_ref, fr_ref, wq_h, wk_h, wv_h, wo_h,
               h_ref, hp_ref,
               xv, csv, snv, wqb, wkb, wvb, wob, qb, kvb, m_s, al_s, acc_s, s0, s1, p0, p1, ob, hs,
               ld, ks, kr, ws, wr, hsem):
    c = lax.axis_index('cp')
    j = lax.axis_index('tp')
    core = lax.rem(c, 2)
    k = c * 2 + j
    cs_ = c + 1 - 2 * core
    cx = lax.rem(c + 2, 4)
    cxs = lax.rem(cs_ + 2, 4)
    SIB = {"cp": cs_}
    XP = {"cp": cx}
    YP = {"tp": 1 - j}
    S = [s0, s1]
    PP = [p0, p1]

    def rc(src, dst, ss, rs, dev):
        return pltpu.make_async_remote_copy(src_ref=src, dst_ref=dst, send_sem=ss, recv_sem=rs, device_id=dev, device_id_type=MESH)

    loads = [(x_h, xv), (wq_h, wqb.at[0]), (wk_h, wkb.at[0]), (wv_h, wvb.at[0])]
    loads = [pltpu.make_async_copy(a, b, ld.at[i]) for i, (a, b) in enumerate(loads)]
    wol = pltpu.make_async_copy(wo_h, wob.at[pl.ds(0, QW)], ld.at[6])
    for l in loads:
        l.start()

    bar = pltpu.get_barrier_semaphore()
    for d in (SIB, XP, YP):
        pl.semaphore_signal(bar, inc=1, device_id=d, device_id_type=MESH)
    pl.semaphore_wait(bar, 3)

    W = {'k': (wk_h, wkb.at[1], 2, 0, 1), 'v': (wv_h, wvb.at[1], 2, 0, 1), 'qa': (wq_h, wqb.at[1], 4, 0, 2),
         'qb': (wq_h, wqb.at[1], 4, 1, 2), 'o': (wo_h, wob.at[pl.ds(QW, QW)], 2, 0, 1)}
    WI = {n: i for i, n in enumerate(W)}

    def wrange(n, q):
        src, dst, div, sub, nsub = W[n]
        r = src.shape[0] // div
        return pl.ds(pl.multiple_of(q * r + sub * (r // nsub), r // nsub), r // nsub)

    def wcopy(n, hop):
        src, dst, div, sub, nsub = W[n]
        q = core if div == 2 else (c if hop < 3 else cx)
        rg = wrange(n, q)
        i = WI[n]
        return rc((src if hop == 0 else dst).at[rg], dst.at[rg], ws.at[i, hop], wr.at[i, hop], (YP, SIB, XP, SIB)[hop])

    def wrecv(n, hop):
        src, dst, div, sub, nsub = W[n]
        q = (core, 1 - core)[hop] if div == 2 else (c, cs_, cx, cxs)[hop]
        rg = wrange(n, q)
        i = WI[n]
        rc(dst.at[rg], dst.at[rg], ws.at[i, hop], wr.at[i, hop], (YP, SIB, XP, SIB)[hop]).wait_recv()

    KV = {'S': '0002S', 'X': '0004X', 'Y': '0011Y', 'XS': '0406S', 'YS': '1113S', 'Z': '1115X', 'ZS': '1517S',
          's': '1012S', 'x': '1014X', 'y': '1001Y', 'xs': '1416S', 'ys': '0103S', 'z': '0105X', 'zs': '0507S'}
    PEER = {'S': SIB, 'X': XP, 'Y': YP}

    def kcopy(n):
        (gs, ms, gd, md), dev = map(int, KV[n][:-1]), PEER[KV[n][-1]]
        return rc(kvb.at[gs, ms], kvb.at[gd, md], ks.at[gd, md], kr.at[gd, md], dev)

    for n in ('k', 'v', 'qa', 'qb'):
        wcopy(n, 0).start()

    sign = jnp.where(lax.broadcasted_iota(jnp.int32, (128, DH), 1) < DH // 2, -1.0, 1.0)

    def table(i, _):
        r = pl.ds(pl.multiple_of(i * 128, 128), 128)
        p = jnp.broadcast_to(pos_ref[pl.ds(i, 1), :].astype(jnp.float32), (128, 128)).T
        ang = p * fr_ref[...]
        csv[r, :] = jnp.cos(ang)
        snv[r, :] = jnp.sin(ang) * sign
        return 0

    lax.fori_loop(0, x_h.shape[0] // 128, table, 0)
    for l in loads:
        l.wait()
    wol.start()

    def front(g, do_q, do_kv):
        def blk(i, _):
            r = pl.ds(pl.multiple_of(i * 256, 256), 256)
            a = rms(xv[r, :], g_ref[...].reshape(1, D))
            ww = ([wqb[g]] if do_q else []) + ([wkb[g], wvb[g]] if do_kv else [])
            y = jnp.dot(a, jnp.concatenate(ww, axis=1) if len(ww) > 1 else ww[0], preferred_element_type=jnp.float32)
            cc = csv[r, :]
            sc = snv[r, :]

            def rot(h):
                u = y[:, h * DH:(h + 1) * DH]
                return (u * cc + pltpu.roll(u, DH // 2, 1) * sc).astype(jnp.bfloat16)

            if do_q:
                for h in range(GRP):
                    qb[g, r, h * DH:(h + 1) * DH] = rot(h)
            if do_kv:
                n = GRP if do_q else 0
                kvb[g, 0, r, :DH] = rot(n)
                kvb[g, 0, r, DH:] = y[:, (n + 1) * DH:(n + 2) * DH].astype(jnp.bfloat16)
            return 0

        lax.fori_loop(0, 4, blk, 0)

    front(0, True, True)
    for n in 'SX':
        kcopy(n).start()

    m_s[...] = jnp.full_like(m_s, NEG)
    acc_s[...] = jnp.zeros_like(acc_s)
    al_s[...] = jnp.ones_like(al_s)
    p1[...] = jnp.zeros_like(p1)
    ones = jnp.ones((PC, 128), jnp.bfloat16)

    EARLY = '000001002023024043044063064100123013033113133053073143163101' + '102153173'
    LATE = '124114134144164154174014034054074'
    NB = len(EARLY) // 3
    codes = [int(c[0]) * 64 + int(c[1]) * 8 + int(c[2]) for c in re.findall('...', EARLY + LATE)]
    NU = len(codes)

    def code_of(u):
        v = jnp.int32(codes[0])
        for i in range(1, NU):
            v = jnp.where(u == i, codes[i], v)
        return v

    def decode(cd):
        g = cd // 64
        m = (cd // 8) % 8
        t = cd % 8
        lt = jnp.where(m >= 4, k // 4, jnp.where(m >= 2, (k // 2) % 2, k % 2))
        qp = jnp.where(t == 0, 0, jnp.where(t == 3, 1 - lt, 1))
        hf = jnp.where(t == 1, 1, jnp.where(t == 4, 1 - lt, 0))
        return g, m, t, qp, hf

    def qk(e, h):
        g, m, t, qp, hf = e
        qo = pl.multiple_of(qp * PC, PC)
        ko = pl.multiple_of(hf * PC, PC)
        S[h % 2][...] = lax.dot_general(qb[g, pl.ds(qo, PC), h * DH:(h + 1) * DH], kvb[g, m, pl.ds(ko, PC), :DH],
                                        (((1,), (1,)), ((), ())), preferred_element_type=jnp.float32)

    def sm(e, h, masked):
        g, m, t, qp, hf = e
        s = S[h % 2][...]
        if masked:
            r = lax.broadcasted_iota(jnp.int32, s.shape, 0)
            cc = lax.broadcasted_iota(jnp.int32, s.shape, 1)
            s = jnp.where(cc <= r, s, NEG)
        mx = jnp.max(s, axis=1, keepdims=True)
        mp = m_s[g, qp, h]
        mn = jnp.maximum(mp, mx)
        al_s[h % 2] = jnp.exp2((mp - mn) * LC)
        pr = jnp.exp2(s * LC - jnp.tile(mn * LC, (1, PC // 128)))
        PP[h % 2][...] = pr.astype(jnp.bfloat16)
        m_s[g, qp, h] = mn

    def pv(e, h):
        g, m, t, qp, hf = e
        ko = pl.multiple_of(hf * PC, PC)
        vb = jnp.concatenate([kvb[g, m, pl.ds(ko, PC), DH:], ones], axis=1)
        y = jnp.dot(PP[h % 2][...], vb, preferred_element_type=jnp.float32)
        acc_s[g, qp, h] = acc_s[g, qp, h] * jnp.tile(al_s[h % 2], (1, 2)) + y

    def finalize(qp):
        def blk(i, _):
            r = pl.ds(pl.multiple_of(i * 256, 256), 256)
            rx = pl.ds(pl.multiple_of(qp * PC + i * 256, 256), 256)
            for g in range(2):
                for h in range(GRP):
                    a = acc_s[g, qp, h, r, :]
                    ob[r, (g * GRP + h) * DH:(g * GRP + h + 1) * DH] = (a[:, :128] / a[:, 128:]).astype(jnp.bfloat16)
            y = jnp.dot(ob[r, :], wob[...], preferred_element_type=jnp.float32)
            hs[rx, :] = (xv[rx, :].astype(jnp.float32) + y).astype(jnp.bfloat16)
            if qp == 0:
                hcopy(i).start()
            return 0

        lax.fori_loop(0, 2, blk, 0)

    def hcopy(i):
        r = pl.ds(pl.multiple_of(i * 256, 256), 256)
        return rc(hs.at[r], hp_ref.at[r], hsem.at[0, i], hsem.at[1, i], YP)

    hout = [pltpu.make_async_copy(hs.at[pl.ds(i * PC, PC)], h_ref.at[pl.ds(i * PC, PC)], ld.at[7 + i]) for i in range(2)]

    kw = lambda n: kcopy(n).wait_recv()

    def act(u, prv):
        def at(i):
            return pl.when(u == i)

        @at(2)
        def _():
            for n in 'kv':
                wrecv(n, 0)
                wcopy(n, 1).start()
            kw('S')

        @at(3)
        def _():
            for n in 'kv':
                wrecv(n, 1)
            front(1, False, True)
            kcopy('s').start()
            kcopy('y').start()
            kcopy('Y').start()

        @at(4)
        def _():
            kw('X')
            kcopy('XS').start()
            wrecv('qa', 0)
            wcopy('qa', 2).start()
            wcopy('qa', 1).start()

        @at(6)
        def _():
            kw('XS')
            wrecv('qb', 0)
            wcopy('qb', 2).start()
            wcopy('qb', 1).start()

        @at(8)
        def _():
            wrecv('qa', 2)
            wcopy('qa', 3).start()
            wrecv('qb', 2)
            wcopy('qb', 3).start()
            kw('y')
            kcopy('ys').start()
            kcopy('z').start()
            for n in ('qa', 'qb'):
                wrecv(n, 1)
                wrecv(n, 3)
            front(1, True, False)

        @at(9)
        def _():
            kcopy('x').start()
            wcopy('o', 0).start()
            kw('s')

        @at(10)
        def _():
            kw('Y')
            kcopy('YS').start()
            kcopy('Z').start()

        @at(11)
        def _():
            kw('ys')

        @at(12)
        def _():
            kw('z')
            kcopy('zs').start()

        @at(13)
        def _():
            kw('YS')

        @at(15)
        def _():
            kw('zs')

        @at(16)
        def _():
            kw('x')
            kcopy('xs').start()

        @at(17)
        def _():
            kw('xs')

        @at(20)
        def _():
            kw('Z')
            kcopy('ZS').start()

        @at(21)
        def _():
            wrecv('o', 0)
            wcopy('o', 1).start()
            kw('ZS')

        @at(NB)
        def _():
            pv(prv, GRP - 1)
            p1[...] = jnp.zeros_like(p1)
            al_s[1] = jnp.ones_like(al_s[1])
            wol.wait()
            wrecv('o', 1)
            finalize(0)
            hout[0].start()

    e0 = decode(jnp.int32(codes[0]))
    qk(e0, 0)

    def body(u, carry):
        cc, pc = carry
        nc = code_of(jnp.minimum(u + 1, NU - 1))
        cur, prv, nxt = decode(cc), decode(pc), decode(nc)
        act(u, prv)

        def run(masked):
            for h in range(GRP):
                if h < GRP - 1:
                    qk(cur, h + 1)
                else:
                    qk(nxt, 0)
                if h == 0:
                    pv(prv, GRP - 1)
                else:
                    pv(cur, h - 1)
                sm(cur, h, masked)

        diag = cur[2] < 2

        @pl.when(diag)
        def _():
            run(True)

        @pl.when(jnp.logical_not(diag))
        def _():
            run(False)

        return nc, cc

    fin = lax.fori_loop(0, NU, body, (jnp.int32(codes[0]), jnp.int32(codes[0])))
    pv(decode(fin[1]), GRP - 1)
    finalize(1)
    hout[1].start()
    for i in range(2):
        hcopy(i).wait_recv()
        hcopy(i).wait_send()
    for o in hout:
        o.wait()
    for n in KV:
        kcopy(n).wait_send()
    for n in W:
        for hop in range(W[n][2]):
            wcopy(n, hop).wait_send()


def att(x, g, pos, fr, wq, wk, wv, wo):
    n = x.shape[0]
    any_ = pl.BlockSpec(memory_space=pl.ANY)
    vm = pl.BlockSpec(memory_space=pltpu.VMEM)
    bf, f32 = jnp.bfloat16, jnp.float32
    return pl.pallas_call(
        att_kernel,
        in_specs=[any_, vm, vm, vm] + [any_] * 4,
        out_specs=[any_, any_],
        out_shape=[jax.ShapeDtypeStruct((n, D), bf), jax.ShapeDtypeStruct((PC, D), bf)],
        scratch_shapes=[
            pltpu.VMEM((n, D), bf), pltpu.VMEM((n, DH), f32), pltpu.VMEM((n, DH), f32),
            pltpu.VMEM((2, D, QW), bf), pltpu.VMEM((2, D, DH), bf), pltpu.VMEM((2, D, DH), bf), pltpu.VMEM((D, D), bf),
            pltpu.VMEM((2, n, QW), bf), pltpu.VMEM((2, 8, n, 2 * DH), bf),
            pltpu.VMEM((2, 2, GRP, PC, 128), f32), pltpu.VMEM((2, PC, 128), f32), pltpu.VMEM((2, 2, GRP, PC, 256), f32),
            pltpu.VMEM((PC, PC), f32), pltpu.VMEM((PC, PC), f32), pltpu.VMEM((PC, PC), bf), pltpu.VMEM((PC, PC), bf),
            pltpu.VMEM((PC, D), bf), pltpu.VMEM((n, D), bf),
            pltpu.SemaphoreType.DMA((9,)), pltpu.SemaphoreType.DMA((2, 8)), pltpu.SemaphoreType.DMA((2, 8)),
            pltpu.SemaphoreType.DMA((5, 4)), pltpu.SemaphoreType.DMA((5, 4)), pltpu.SemaphoreType.DMA((2, 2))],
        compiler_params=pltpu.CompilerParams(collective_id=0, has_side_effects=True, vmem_limit_bytes=VM),
        cost_estimate=cost(70e9, 20 * 2**20), name="att")(x, g, pos, fr, wq, wk, wv, wo)


FU = 896
ND = 768


def mlp_kernel(h_h, hpb_h, g_ref, w1_h, w3_h, w2_h, ob_h, oa_h, hall, wb, w2b, hid, b_s, zs, zr, zo, ld, us, ds, os_, zsem, zrm):
    j = lax.axis_index('tp')
    YP = {"tp": 1 - j}
    F = w1_h.shape[1]
    NU_, NDN = F // FU, D // ND

    def rc(src, dst, ss, rs):
        return pltpu.make_async_remote_copy(src_ref=src, dst_ref=dst, send_sem=ss, recv_sem=rs, device_id=YP, device_id_type=MESH)

    def up(t, slot):
        o = pl.multiple_of(t * FU, 128)
        return [pltpu.make_async_copy(w1_h.at[:, pl.ds(o, FU)], wb.at[slot, :, pl.ds(0, FU)], us.at[slot, 0]),
                pltpu.make_async_copy(w3_h.at[:, pl.ds(o, FU)], wb.at[slot, :, pl.ds(FU, FU)], us.at[slot, 1])]

    def down(t, slot):
        return pltpu.make_async_copy(w2_h.at[:, pl.ds(pl.multiple_of(t * ND, 128), ND)], w2b.at[slot], ds.at[slot])

    hl = [pltpu.make_async_copy(hpb_h, hall.at[2], ld.at[0]),
          pltpu.make_async_copy(h_h.at[pl.ds(0, PC)], hall.at[0], ld.at[1]),
          pltpu.make_async_copy(h_h.at[pl.ds(PC, PC)], hall.at[1], ld.at[2])]
    hl[0].start()
    for cp in up(0, 0):
        cp.start()
    for cp in hl[1:]:
        cp.start()

    bar = pltpu.get_barrier_semaphore()
    pl.semaphore_signal(bar, inc=1, device_id=YP, device_id_type=MESH)
    pl.semaphore_wait(bar, 1)
    hsend = rc(h_h.at[pl.ds(PC, PC)], hall.at[3], zsem.at[2], zrm.at[2])
    hsend.start()
    hp = PC // 2
    zc = [rc(zs.at[0], zr.at[0], zsem.at[0], zrm.at[0])]
    zc = zc + [rc(zs.at[1, pl.ds(i * hp, hp)], zr.at[1, pl.ds(i * hp, hp)], zsem.at[(1, 3)[i]], zrm.at[(1, 3)[i]]) for i in range(2)]
    outs = (ob_h, oa_h)
    oc = [pltpu.make_async_copy(hall.at[i, pl.ds(r, hp)], outs[i].at[pl.ds(r, hp)], os_.at[i, r // hp]) for i in range(2) for r in (0, hp)]

    def finish(i, part):
        def blk(t, _):
            r = pl.ds(pl.multiple_of(part * hp + t * 128, 128), 128)
            y = hall[i, r, :].astype(jnp.float32) + (zo[i, r, :] + zr[i, r, :].astype(jnp.float32))
            hall[i, r, :] = y.astype(jnp.bfloat16)
            return 0

        lax.fori_loop(0, hp // 128, blk, 0)
        oc[2 * i + part].start()

    def up_phase(n, idx, hb, more, pre):
        b_s[...] = rms(hall[idx], g_ref[...].reshape(1, D))

        def step(t, _):
            slot = (n * NU_ + t) % 2
            last = t == NU_ - 1

            @pl.when(jnp.logical_or(more, jnp.logical_not(last)))
            def _():
                for cp in up(jnp.where(last, 0, t + 1), 1 - slot):
                    cp.start()

            if pre is not None:
                @pl.when(t == NU_ - 2)
                def _():
                    down(0, pre).start()

            for cp in up(t, slot):
                cp.wait()
            y = jnp.dot(b_s[...], wb[slot], preferred_element_type=jnp.float32)
            a = y[:, :FU]
            hid[hb, :, pl.ds(pl.multiple_of(t * FU, 128), FU)] = (a * jax.nn.sigmoid(a) * y[:, FU:]).astype(jnp.bfloat16)
            return 0

        lax.fori_loop(0, NU_, step, 0)

    def down_phase(n, idx, hb, chain):
        def step(t, _):
            slot = (n * NDN + t) % 2

            @pl.when(jnp.logical_or(chain, t < NDN - 1))
            def _():
                down(jnp.where(t == NDN - 1, 0, t + 1), 1 - slot).start()

            down(t, slot).wait()
            y = jnp.dot(hid[hb], w2b[slot], preferred_element_type=jnp.float32)
            cols = pl.ds(pl.multiple_of(t * ND, 128), ND)
            if idx >= 2:
                zs[idx - 2, :, cols] = y.astype(jnp.bfloat16)
            else:
                zo[idx, :, cols] = y
            return 0

        lax.fori_loop(0, NDN, step, 0)

    hl[0].wait()
    up_phase(0, 2, 0, True, 0)
    down_phase(0, 2, 0, False)
    hl[1].wait()
    zc[0].start()
    up_phase(1, 0, 1, True, None)
    hsend.wait_recv()
    up_phase(2, 3, 0, True, NDN % 2)
    down_phase(1, 3, 0, True)
    zc[1].start()
    zc[2].start()
    down_phase(2, 0, 1, False)
    zc[0].wait_recv()
    finish(0, 0)
    finish(0, 1)
    hl[2].wait()
    up_phase(3, 1, 0, False, (3 * NDN) % 2)
    down_phase(3, 1, 0, False)
    for i in range(2):
        zc[1 + i].wait_recv()
        finish(1, i)
    for o in oc:
        o.wait()
    hsend.wait_send()
    for z in zc:
        z.wait_send()


def mlp(h, hpb, g, w1, w3, w2):
    n = h.shape[0]
    f = w1.shape[1]
    any_ = pl.BlockSpec(memory_space=pl.ANY)
    bf, f32 = jnp.bfloat16, jnp.float32
    return pl.pallas_call(
        mlp_kernel,
        in_specs=[any_, any_, pl.BlockSpec(memory_space=pltpu.VMEM), any_, any_, any_],
        out_specs=[any_] * 2,
        out_shape=[jax.ShapeDtypeStruct((PC, D), bf)] * 2,
        scratch_shapes=[
            pltpu.VMEM((4, PC, D), bf), pltpu.VMEM((2, D, 2 * FU), bf), pltpu.VMEM((2, f, ND), bf),
            pltpu.VMEM((2, PC, f), bf), pltpu.VMEM((PC, D), bf), pltpu.VMEM((2, PC, D), bf), pltpu.VMEM((2, PC, D), bf),
            pltpu.VMEM((2, PC, D), f32),
            pltpu.SemaphoreType.DMA((3,)), pltpu.SemaphoreType.DMA((2, 2)), pltpu.SemaphoreType.DMA((2,)), pltpu.SemaphoreType.DMA((2, 2)),
            pltpu.SemaphoreType.DMA((4,)), pltpu.SemaphoreType.DMA((4,))],
        compiler_params=pltpu.CompilerParams(collective_id=1, has_side_effects=True, vmem_limit_bytes=VM),
        cost_estimate=cost(12 * n * D * f, 24 * D * f), name="mlp")(h, hpb, g, w1, w3, w2)


def solution(mesh):
    tok = P(('dp', 'cp', 'tp'), None)
    col = P(None, 'tp')
    row = P('tp', None)

    def local(x, pos, g1, g2, wq, wk, wv, wo, w1, w3, w2):
        fr = 1.0 / (np.float32(THETA) ** (np.arange(0, DH, 2, dtype=np.float32) / np.float32(DH)))
        fr = jnp.asarray(np.concatenate([fr, fr]).astype(np.float32).reshape(1, DH))
        h, hp = att(x, g1, pos.reshape(-1, 128), fr, wq, wk, wv, wo)
        return jnp.concatenate(mlp(h, hp, g2, w1, w3, w2), 0)

    return jax.shard_map(local, mesh=mesh, in_specs=(tok, P(('dp', 'cp', 'tp')), P(None), P(None), col, col, col, row, col, col, row), out_specs=tok, check_vma=False)
```
